64 devices in a mesh: dp: 4 (over x, y), wg: 16 (over z, core).
Axes of the slice: x: 2, y: 2, z: 8, core: 2. Of those that a mesh axis runs over, the one named last changes fastest.
The devices are a block of a 4x4x8 slice.
Arguments:
- hidden: bfloat16 [65536, 1024], P(('dp', 'wg')), parts along dimension 0
- choice: int32 [65536, 8], P(('dp', 'wg')), parts along dimension 0
- pre_scale: float32 [1024], replicated
- w_router: bfloat16 [1024, 32], replicated
- w_gelu: bfloat16 [32, 1024, 512], P(None, None, 'wg')
- w_linear: bfloat16 [32, 1024, 512], P(None, None, 'wg')
- w_down: bfloat16 [32, 512, 1024], P(None, 'wg')
- post_scale: float32 [1024], replicated
Outputs:
- output: bfloat16 [65536, 1024], P(('dp', 'wg')), parts along dimension 0
There are 4 independent parts. The reference program is written for one: setup_inputs(seed, part) draws one part's arguments, and reference() takes and returns one part's arrays. A program takes and returns all parts, laid end to end along the dimension named above; an argument that names none is the same for every part.
All inputs are finite; a program needn't handle non-finite values.
Results may differ from the reference program's by a relative error of at most 0.001.
Values are sent between devices in bfloat16 or wider.
A program may use at most 768 MiB of HBM per device.

```python
import jax
import jax.numpy as jnp
from jax import lax

D_MODEL = 1024
D_FF = 512
EXPERTS = 32
TOP_K = 8
TOKENS_DEV = 1024
GROUP_DEVS = 16
EPS = 1e-5


def block_choice(block_key):
    mean_load = TOKENS_DEV * TOP_K // EXPERTS
    key_perm, key_delta, key_rows = jax.random.split(block_key, 3)
    expert_perm = jax.random.permutation(key_perm, EXPERTS)
    pair_delta = jax.random.randint(key_delta, (EXPERTS,), 0, mean_load)
    position = jnp.arange(EXPERTS)
    pair_index = jnp.maximum((position - 3) // 2, 0)
    pair_sign = jnp.where((position - 3) % 2 == 0, 1, -1)
    paired = (position >= 3) & (4 + 2 * pair_index < EXPERTS)
    load_delta = jnp.where(paired, pair_sign * pair_delta[pair_index], 0)
    load_delta = load_delta + jnp.where(position == 0, mean_load, 0) - jnp.where((position == 1) | (position == 2), mean_load // 2, 0)
    expert_loads = mean_load + load_delta
    run_ends = jnp.cumsum(expert_loads)
    flat_pos = jnp.arange(TOKENS_DEV * TOP_K)
    run_index = jnp.sum((flat_pos[:, None] >= run_ends[None, :]).astype(jnp.int32), axis=1)
    choice_grid = expert_perm[run_index].reshape(TOP_K, TOKENS_DEV).T
    row_perm = jax.random.permutation(key_rows, TOKENS_DEV)
    return choice_grid[row_perm].astype(jnp.int32)


def setup_inputs(seed: int = 0, part: int = 0) -> dict:
    weight_keys = jax.random.split(jax.random.key(seed), 6)
    part_key = jax.random.fold_in(jax.random.key(seed + 1), part)
    key_hidden, key_choice = jax.random.split(part_key)
    row_count = GROUP_DEVS * TOKENS_DEV
    hidden = jax.random.normal(key_hidden, (row_count, D_MODEL), jnp.float32).astype(jnp.bfloat16)
    choice = jax.vmap(block_choice)(jax.random.split(key_choice, GROUP_DEVS)).reshape(row_count, TOP_K)
    pre_scale = 1.0 + 0.5 * jax.random.normal(weight_keys[0], (D_MODEL,), jnp.float32)
    w_router = (jax.random.normal(weight_keys[1], (D_MODEL, EXPERTS), jnp.float32) * D_MODEL ** -0.5).astype(jnp.bfloat16)
    w_gelu = (jax.random.normal(weight_keys[2], (EXPERTS, D_MODEL, D_FF), jnp.float32) * D_MODEL ** -0.5).astype(jnp.bfloat16)
    w_linear = (jax.random.normal(weight_keys[3], (EXPERTS, D_MODEL, D_FF), jnp.float32) * D_MODEL ** -0.5).astype(jnp.bfloat16)
    w_down = (jax.random.normal(weight_keys[4], (EXPERTS, D_FF, D_MODEL), jnp.float32) * D_FF ** -0.5).astype(jnp.bfloat16)
    post_scale = 1.0 + 0.5 * jax.random.normal(weight_keys[5], (D_MODEL,), jnp.float32)
    return dict(hidden=hidden, choice=choice, pre_scale=pre_scale, w_router=w_router, w_gelu=w_gelu, w_linear=w_linear, w_down=w_down, post_scale=post_scale)


def rms_norm(values, gain_vec):
    return values * lax.rsqrt(jnp.mean(values * values, axis=-1, keepdims=True) + EPS) * gain_vec


def route_slots(block_ids, capacity):
    tok_rows, top_k = block_ids.shape
    flat_ids = block_ids.reshape(-1)
    sort_order = jnp.argsort(flat_ids, stable=True)
    counts = jnp.sum((flat_ids[:, None] == jnp.arange(EXPERTS)[None, :]).astype(jnp.int32), axis=0)
    starts = jnp.cumsum(counts) - counts
    slot_rank = jnp.arange(capacity)
    source = jnp.minimum(starts[:, None] + slot_rank[None, :], tok_rows * top_k - 1)
    slot_token = sort_order[source].reshape(-1) // top_k
    sorted_pos = jnp.argsort(sort_order, stable=True)
    slot_of = flat_ids * capacity + sorted_pos - starts[flat_ids]
    return slot_token, slot_of


def reference(hidden, choice, pre_scale, w_router, w_gelu, w_linear, w_down, post_scale):
    capacity = 2 * TOKENS_DEV * TOP_K // EXPERTS
    hidden_f = hidden.astype(jnp.float32)
    normed = rms_norm(hidden_f, pre_scale).astype(jnp.bfloat16)
    router_probs = jax.nn.softmax(jnp.dot(normed, w_router, preferred_element_type=jnp.float32), axis=-1)
    gate_vals = jnp.take_along_axis(router_probs, choice, axis=1)

    def one_expert(expert_args):
        expert_rows, gelu_w, linear_w, down_w = expert_args
        gelu_in = jnp.dot(expert_rows, gelu_w, preferred_element_type=jnp.float32)
        linear_in = jnp.dot(expert_rows, linear_w, preferred_element_type=jnp.float32)
        hidden_act = (jax.nn.gelu(gelu_in, approximate=True) * linear_in).astype(jnp.bfloat16)
        return jnp.dot(hidden_act, down_w, preferred_element_type=jnp.float32)

    def one_block(block_args):
        block_rows, block_ids, block_gates = block_args
        slot_token, slot_of = route_slots(block_ids, capacity)
        dispatched = jnp.take(block_rows, slot_token, axis=0).reshape(EXPERTS, capacity, D_MODEL)
        expert_out = lax.map(one_expert, (dispatched, w_gelu, w_linear, w_down)).reshape(EXPERTS * capacity, D_MODEL)
        picked = jnp.take(expert_out, slot_of, axis=0).reshape(TOKENS_DEV, TOP_K, D_MODEL)
        return jnp.sum(picked * block_gates[:, :, None], axis=1)

    mixed_out = lax.map(one_block, (normed.reshape(GROUP_DEVS, TOKENS_DEV, D_MODEL), choice.reshape(GROUP_DEVS, TOKENS_DEV, TOP_K), gate_vals.reshape(GROUP_DEVS, TOKENS_DEV, TOP_K))).reshape(GROUP_DEVS * TOKENS_DEV, D_MODEL)
    return (hidden_f + rms_norm(mixed_out, post_scale)).astype(jnp.bfloat16)
```

```python
import functools
import math

import jax
import jax.numpy as jnp
from jax import lax
from jax.experimental import pallas as pl
from jax.experimental.pallas import tpu as pltpu
from jax.sharding import PartitionSpec as P

EPS = 1e-5
MESH = pl.DeviceIdType.MESH
VMEM_BYTES = 67_043_328


def dot_t(lhs, rhs):
    return lax.dot_general(lhs, rhs, (((1,), (1,)), ((), ())), preferred_element_type=jnp.float32)


def moe_kernel(side, chips, blk, hid_ref, choice_ref, pre_ref, router_ref, wg_ref, wl_ref, wd_ref, own_out, part_out,
               wts, rows, acc, gates, up_ss, up_rs, dn_ss, dn_rs, x_ss, x_rs, y_ss, y_rs, load_sem, sib_ss, sib_rs, part_ss, part_rs):
    tok, d_model = hid_ref.shape
    experts, _, _, shard, _ = wts.shape
    width = chips * shard
    rounds = experts // 4
    far = chips // 2
    near = chips - 1 - far
    slots = chips - 1
    nblk = tok // blk
    ncol = min(256, d_model)

    dp, wg = lax.axis_index('dp'), lax.axis_index('wg')
    z, core = wg // 2, wg % 2
    sib = wg + 1 - 2 * core
    up = ((z + 1) % chips) * 2 + core
    down = ((z + chips - 1) % chips) * 2 + core
    gx, gy = dp // side, dp % side
    xdp = dp + side * (1 - 2 * (gx % 2))
    ydp = dp + 1 - 2 * (gy % 2)
    par = (gx + gy) % 2

    def remote(ref, ss, rs, where, h, s):
        return pltpu.make_async_remote_copy(src_ref=ref, dst_ref=ref, send_sem=ss.at[h, s - 1], recv_sem=rs.at[h, s - 1],
                                            device_id=where, device_id_type=MESH)

    def mine(h):
        return 2 * h + par

    def theirs(h):
        return 2 * h + 1 - par

    def behind(s):
        return (z - s + chips) % chips

    def ahead(s):
        return (z + s) % chips

    def up_send(h, s):
        return remote(wts.at[mine(h), behind(s - 1)], up_ss, up_rs, (dp, up), h, s)

    def up_recv(h, s):
        return remote(wts.at[mine(h), behind(s)], up_ss, up_rs, (dp, up), h, s)

    def dn_send(h, s):
        return remote(wts.at[mine(h), ahead(s - 1)], dn_ss, dn_rs, (dp, down), h, s)

    def dn_recv(h, s):
        return remote(wts.at[mine(h), ahead(s)], dn_ss, dn_rs, (dp, down), h, s)

    def x_send(h, s):
        return remote(wts.at[mine(h), behind(s)], x_ss, x_rs, (xdp, wg), h, s)

    def x_recv(h, s):
        return remote(wts.at[theirs(h), behind(s)], x_ss, x_rs, (xdp, wg), h, s)

    def y_send(h, s):
        return remote(wts.at[mine(h), ahead(s)], y_ss, y_rs, (ydp, wg), h, s)

    def y_recv(h, s):
        return remote(wts.at[theirs(h), ahead(s)], y_ss, y_rs, (ydp, wg), h, s)

    def sibling(src, dst, k):
        return pltpu.make_async_remote_copy(src_ref=src, dst_ref=dst, send_sem=sib_ss.at[k], recv_sem=sib_rs.at[k],
                                            device_id=(dp, sib), device_id_type=MESH)

    def partial_sum(c):
        return pltpu.make_async_remote_copy(src_ref=acc.at[1, pl.ds(c * blk, blk)], dst_ref=part_out.at[pl.ds(c * blk, blk)],
                                            send_sem=part_ss.at[c], recv_sem=part_rs.at[c], device_id=(dp, sib), device_id_type=MESH)

    loads = []
    for k, src in enumerate((wg_ref, wl_ref, wd_ref)):
        loads.append(pltpu.make_async_copy(src.at[pl.ds(0, 4)], wts.at[pl.ds(0, 4), z, k], load_sem.at[k]))
    for k, src in enumerate((wg_ref, wl_ref, wd_ref)):
        loads.append(pltpu.make_async_copy(src.at[pl.ds(4, experts - 4)], wts.at[pl.ds(4, experts - 4), z, k], load_sem.at[3 + k]))
    loads.append(pltpu.make_async_copy(hid_ref, rows.at[0], load_sem.at[6]))
    for load in loads:
        load.start()

    barrier = pltpu.get_barrier_semaphore()
    for peer in ((dp, up), (dp, down), (xdp, wg), (ydp, wg), (dp, sib)):
        pl.semaphore_signal(barrier, inc=1, device_id=peer, device_id_type=MESH)
    pl.semaphore_wait(barrier, 5)

    for load in loads[:3]:
        load.wait()
    up_send(0, 1).start()
    dn_send(1, 1).start()
    up_send(1, 1).start()
    dn_send(0, 1).start()

    loads[6].wait()
    nrm = min(128, tok)

    @pl.loop(0, tok // nrm)
    def _(i):
        at = pl.ds(pl.multiple_of(i * nrm, nrm), nrm)
        values = rows[0, at, :].astype(jnp.float32)
        scale = lax.rsqrt(jnp.mean(values * values, axis=-1, keepdims=True) + EPS)
        rows[0, at, :] = (values * scale * pre_ref[...]).astype(jnp.bfloat16)

    for load in loads[3:6]:
        load.wait()

    rtr = min(256, tok)

    @pl.loop(0, tok // rtr)
    def _(i):
        at = pl.ds(pl.multiple_of(i * rtr, rtr), rtr)
        logits = dot_t(router_ref[...], rows[0, at, :])
        shifted = jnp.exp(logits - jnp.max(logits, axis=0, keepdims=True))
        probs = shifted / jnp.sum(shifted, axis=0, keepdims=True)
        expert_ids = lax.broadcasted_iota(jnp.int32, (experts, rtr), 0)
        picks = choice_ref[:, at]
        chosen = expert_ids == picks[0:1, :]
        for j in range(1, picks.shape[0]):
            chosen = chosen | (expert_ids == picks[j:j + 1, :])
        gates[0, at, :] = jnp.where(chosen, probs, -1.0).T

    @pl.loop(0, 2 * tok // nrm)
    def _(i):
        at = pl.ds(pl.multiple_of((i // 2) * nrm, nrm), nrm)
        acc[i % 2, at, :] = jnp.zeros((nrm, d_model), jnp.float32)

    rows_copy = sibling(rows.at[0], rows.at[1], 0)
    gates_copy = sibling(gates.at[0], gates.at[1], 1)
    rows_copy.start()
    gates_copy.start()

    def exchange(r, j, more):
        even, odd = 2 * r, 2 * r + 1
        s = j // 2 + 1
        h_up, n_up = (even, far) if j % 2 == 0 else (odd, near)
        h_dn, n_dn = (odd, far) if j % 2 == 0 else (even, near)
        up_recv(h_up, s).wait_recv()
        if s < n_up:
            up_send(h_up, s + 1).start()
        elif more is not None:
            more(lambda: up_send(even + 2 if j == slots - 2 else odd + 2, 1).start())
        x_send(h_up, s).start()
        dn_recv(h_dn, s).wait_recv()
        if s < n_dn:
            dn_send(h_dn, s + 1).start()
        elif more is not None:
            more(lambda: dn_send(odd + 2 if j == slots - 2 else even + 2, 1).start())
        y_send(h_dn, s).start()

    def arrived(r):
        for h, n_up, n_dn in ((2 * r, far, near), (2 * r + 1, near, far)):
            for s in range(1, n_up + 1):
                x_recv(h, s).wait_recv()
            for s in range(1, n_dn + 1):
                y_recv(h, s).wait_recv()

    def work(r, q):
        odd = q % 2
        rb = (q // 2) % nblk
        half = 1 - (q // (2 * nblk)) % 2
        other = q // (4 * nblk)
        e = 4 * r + 2 * odd + par + other * (1 - 2 * par)
        at = pl.ds(pl.multiple_of(rb * blk, blk), blk)
        x = rows[half, at, :]
        lane = lax.broadcasted_iota(jnp.int32, (blk, experts), 1)
        gate = jnp.sum(jnp.where(lane == e, gates[half, at, :], 0.0), axis=1, keepdims=True)
        u = dot_t(x, wts[e, :, 0].reshape(width, d_model))
        v = dot_t(x, wts[e, :, 1].reshape(width, d_model))
        c = math.sqrt(2.0 / math.pi)
        cdf = 0.5 * (1.0 + jnp.tanh(c * (u + 0.044715 * (u * u * u))))
        a = jnp.where(gate >= 0.0, u * cdf * v, 0.0).astype(jnp.bfloat16)
        for n in range(d_model // ncol):
            cols = pl.ds(n * ncol, ncol)
            o = jnp.dot(a, wts[e, :, 2, :, cols].reshape(width, ncol), preferred_element_type=jnp.float32)
            acc[half, at, cols] += gate * o

    total = 8 * nblk
    cuts = [(total * j + slots - 1) // slots for j in range(slots + 1)]

    for j in range(slots):
        exchange(0, j, (lambda f: f()) if rounds > 1 else None)
    rows_copy.wait_recv()
    gates_copy.wait_recv()

    @pl.loop(1, rounds)
    def _(r):
        waited = False
        for j in range(slots):
            exchange(r, j, lambda f: pl.when(r < rounds - 1)(f))
            if not waited and cuts[j + 1] > total // 2:
                arrived(r - 1)
                waited = True

            @pl.loop(cuts[j], cuts[j + 1])
            def _(q):
                work(r - 1, q)

    last = rounds - 1

    @pl.loop(0, total // 2)
    def _(q):
        work(last, q)

    arrived(last)

    @pl.loop(total // 2, 3 * total // 4)
    def _(q):
        work(last, q)

    for c in range(nblk):
        partial_sum(c).start()

    @pl.loop(3 * total // 4, total)
    def _(q):
        work(last, q)

    own = pltpu.make_async_copy(acc.at[0], own_out, load_sem.at[6])
    own.start()

    @pl.loop(0, rounds)
    def _(r):
        for h, n_up, n_dn in ((2 * r, far, near), (2 * r + 1, near, far)):
            for s in range(1, n_up + 1):
                up_send(h, s).wait_send()
                x_send(h, s).wait_send()
            for s in range(1, n_dn + 1):
                dn_send(h, s).wait_send()
                y_send(h, s).wait_send()

    rows_copy.wait_send()
    gates_copy.wait_send()
    for c in range(nblk):
        partial_sum(c).wait()
    own.wait()


def solution(mesh):
    side = math.isqrt(mesh.shape['dp'])
    chips = mesh.shape['wg'] // 2

    def local_block(hidden, choice, pre_scale, w_router, w_gelu, w_linear, w_down, post_scale):
        tok, d_model = hidden.shape
        experts, _, shard = w_gelu.shape
        blk = min(512, tok // 2)
        half_rounds = experts // 2
        steps = chips // 2
        flow = [pltpu.SemaphoreType.DMA((half_rounds, steps)) for _ in range(8)]
        flops = 2 * 2 * tok * experts * 3 * (chips * shard) * d_model
        own, part = pl.pallas_call(
            functools.partial(moe_kernel, side, chips, blk),
            out_shape=(jax.ShapeDtypeStruct((tok, d_model), jnp.float32), jax.ShapeDtypeStruct((tok, d_model), jnp.float32)),
            in_specs=[
                pl.BlockSpec(memory_space=pl.ANY),
                pl.BlockSpec(memory_space=pltpu.VMEM),
                pl.BlockSpec(memory_space=pltpu.VMEM),
                pl.BlockSpec(memory_space=pltpu.VMEM),
                pl.BlockSpec(memory_space=pl.ANY),
                pl.BlockSpec(memory_space=pl.ANY),
                pl.BlockSpec(memory_space=pl.ANY),
            ],
            out_specs=(pl.BlockSpec(memory_space=pl.ANY), pl.BlockSpec(memory_space=pl.ANY)),
            scratch_shapes=[
                pltpu.VMEM((experts, chips, 3, shard, d_model), jnp.bfloat16),
                pltpu.VMEM((2, tok, d_model), jnp.bfloat16),
                pltpu.VMEM((2, tok, d_model), jnp.float32),
                pltpu.VMEM((2, tok, experts), jnp.float32),
                *flow,
                pltpu.SemaphoreType.DMA((7,)),
                pltpu.SemaphoreType.DMA((2,)),
                pltpu.SemaphoreType.DMA((2,)),
                pltpu.SemaphoreType.DMA((tok // blk,)),
                pltpu.SemaphoreType.DMA((tok // blk,)),
            ],
            compiler_params=pltpu.CompilerParams(collective_id=0, has_side_effects=True, vmem_limit_bytes=VMEM_BYTES),
            cost_estimate=pl.CostEstimate(flops=flops, bytes_accessed=8 * experts * chips * shard * d_model, transcendentals=0),
        )(hidden, choice.T, pre_scale.reshape(1, d_model), w_router.T, jnp.swapaxes(w_gelu, 1, 2), jnp.swapaxes(w_linear, 1, 2), w_down)
        mixed = own + part
        scaled = mixed * lax.rsqrt(jnp.mean(mixed * mixed, axis=-1, keepdims=True) + EPS) * post_scale
        return (hidden.astype(jnp.float32) + scaled).astype(jnp.bfloat16)

    row_spec = P(('dp', 'wg'), None)
    weight_in = P(None, None, 'wg')
    return jax.shard_map(local_block, mesh=mesh, in_specs=(row_spec, row_spec, P(), P(), weight_in, weight_in, P(None, 'wg', None), P()), out_specs=row_spec, check_vma=False)
```

```python
import functools
import math

import jax
import jax.numpy as jnp
from jax import lax
from jax.experimental import pallas as pl
from jax.experimental.pallas import tpu as pltpu
from jax.sharding import PartitionSpec as P

EPS = 1e-5
MESH = pl.DeviceIdType.MESH
VMEM_BYTES = 67_043_328


def dot_t(lhs, rhs):
    return lax.dot_general(lhs, rhs, (((1,), (1,)), ((), ())), preferred_element_type=jnp.float32)


def exclusive_experts(experts):
    count = experts * 11 // 32
    while (experts - count) % 3:
        count -= 1
    return count


def moe_kernel(side, chips, blk, excl, hid_ref, choice_ref, pre_ref, router_ref, wg_ref, wl_ref, wd_ref, own_out, part_out, cross_out, fold_out,
               wts, rows, acc, gate_t, gates, tmp, up_ss, up_rs, dn_ss, dn_rs, y_ss, y_rs, load_sem, row_ss, row_rs, gate_ss, gate_rs,
               fold_ss, fold_rs, cross_ss, cross_rs, part_ss, part_rs):
    tok, d_model = hid_ref.shape
    held, _, _, shard, _ = wts.shape
    experts = held + excl
    width = chips * shard
    slots = chips - 1
    rounds = held // 3
    count = rounds * slots
    nblk = tok // blk
    ncol = min(256, d_model)

    dp, wg = lax.axis_index('dp'), lax.axis_index('wg')
    z, core = wg // 2, wg % 2
    gx, gy = dp // side, dp % side
    px, py = gx % 2, gy % 2
    up = (dp, ((z + 1) % chips) * 2 + core)
    down = (dp, ((z + chips - 1) % chips) * 2 + core)
    sib = (dp, wg + 1 - 2 * core)
    cross = (dp + side * (1 - 2 * px), wg)
    along = (dp + 1 - 2 * py, wg)

    def remote(src, dst, ss, rs, where):
        return pltpu.make_async_remote_copy(src_ref=src, dst_ref=dst, send_sem=ss, recv_sem=rs, device_id=where, device_id_type=MESH)

    def mine(r):
        return 3 * r + 2 * py

    def slice_copy(i, chip, ss, rs, m, where):
        ref = wts.at[i, chip]
        return remote(ref, ref, ss.at[m], rs.at[m], where)

    def up_copy(m, back):
        r, j = m // slots, m % slots
        odd, s = j % 2, j // 2 + 1
        i = 3 * r + (1 - odd) * 2 * py + odd
        return slice_copy(i, (z - s + back + chips) % chips, up_ss, up_rs, m, up)

    def dn_copy(m, back):
        r, j = m // slots, m % slots
        odd, s = j % 2, j // 2 + 1
        i = 3 * r + odd * 2 * py + (1 - odd)
        return slice_copy(i, (z + s - back) % chips, dn_ss, dn_rs, m, down)

    def y_copy(m, i):
        r, j = m // slots, m % slots
        odd, s = j % 2, j // 2 + 1
        return slice_copy(3 * r + i, (z + (2 * odd - 1) * s + chips) % chips, y_ss, y_rs, m, along)

    def exchange(m, more=True):
        up_copy(m, 0).wait_recv()
        if more is True:
            up_copy(m + 2, 1).start()
        else:
            pl.when(m + 2 < count)(lambda: up_copy(m + 2, 1).start())
        dn_copy(m, 0).wait_recv()
        if more is True:
            dn_copy(m + 2, 1).start()
        else:
            pl.when(m + 2 < count)(lambda: dn_copy(m + 2, 1).start())
        y_copy(m, 2 * py).start()

    def partner_slices(r):
        @pl.loop(0, slots)
        def _(k):
            y_copy(r * slots + k, 2 - 2 * py).wait_recv()

    def row_copy(k, where):
        return remote(rows.at[0] if k < 3 else rows.at[2], rows.at[k], row_ss.at[k - 1], row_rs.at[k - 1], where)

    def gate_copy(k, where):
        return remote(gate_t.at[0] if k < 3 else gate_t.at[2], gate_t.at[k], gate_ss.at[k - 1], gate_rs.at[k - 1], where)

    def sum_copy(k, dst, ss, rs, c, where):
        at = pl.ds(c * blk, blk)
        return remote(acc.at[k, at], dst.at[at], ss.at[c], rs.at[c], where)

    loads = []
    for n, (src0, dst0, size) in enumerate(((px * excl, 0, 3), (px * excl + 3, 3, excl - 3), (2 * excl, excl, held - excl)) if excl > 3 else
                                           ((px * excl, 0, excl), (2 * excl, excl, held - excl))):
        for k, src in enumerate((wg_ref, wl_ref, wd_ref)):
            loads.append(pltpu.make_async_copy(src.at[pl.ds(src0, size)], wts.at[pl.ds(dst0, size), z, k], load_sem.at[3 * n + k]))
    hid_load = pltpu.make_async_copy(hid_ref, rows.at[0], load_sem.at[9])
    for load in loads[:3] + [hid_load] + loads[3:]:
        load.start()

    barrier = pltpu.get_barrier_semaphore()
    for peer in (up, down, sib, cross, along):
        pl.semaphore_signal(barrier, inc=1, device_id=peer, device_id_type=MESH)
    pl.semaphore_wait(barrier, 5)

    head = 3 if excl > 3 else 6
    for load in loads[:head]:
        load.wait()
    for m in range(2):
        up_copy(m, 1).start()
        dn_copy(m, 1).start()

    hid_load.wait()
    nrm = min(128, tok)

    @pl.loop(0, tok // nrm)
    def _(i):
        at = pl.ds(pl.multiple_of(i * nrm, nrm), nrm)
        values = rows[0, at, :].astype(jnp.float32)
        scale = lax.rsqrt(jnp.mean(values * values, axis=-1, keepdims=True) + EPS)
        rows[0, at, :] = (values * scale * pre_ref[...]).astype(jnp.bfloat16)

    for load in loads[head:]:
        load.wait()

    rtr = min(256, tok)

    @pl.loop(0, tok // rtr)
    def _(i):
        at = pl.ds(pl.multiple_of(i * rtr, rtr), rtr)
        logits = dot_t(router_ref[...], rows[0, at, :])
        shifted = jnp.exp(logits - jnp.max(logits, axis=0, keepdims=True))
        probs = shifted / jnp.sum(shifted, axis=0, keepdims=True)
        expert_ids = lax.broadcasted_iota(jnp.int32, (experts, rtr), 0)
        picks = choice_ref[:, at]
        chosen = expert_ids == picks[0:1, :]
        for j in range(1, picks.shape[0]):
            chosen = chosen | (expert_ids == picks[j:j + 1, :])
        gate_t[0, :, at] = jnp.where(chosen, probs, -1.0)

    @pl.loop(0, 4 * tok // nrm)
    def _(i):
        at = pl.ds(pl.multiple_of((i // 4) * nrm, nrm), nrm)
        acc[i % 4, at, :] = jnp.zeros((nrm, d_model), jnp.float32)

    for k, where in ((2, cross), (1, sib)):
        gate_copy(k, where).start()
        row_copy(k, where).start()

    def spread_gates(k):
        gates[k] = gate_t[k].T

    spread_gates(0)

    @pl.loop(0, slots)
    def _(j):
        exchange(j)

    row_copy(1, sib).wait_recv()
    gate_copy(1, sib).wait_recv()
    spread_gates(1)

    def work(i, k, rb):
        e = i + excl * (px + (1 - px) * jnp.minimum(i // excl, 1))
        at = pl.ds(pl.multiple_of(rb * blk, blk), blk)
        x = rows[k, at, :]
        lane = lax.broadcasted_iota(jnp.int32, (blk, experts), 1)
        gate = jnp.sum(jnp.where(lane == e, gates[k, at, :], 0.0), axis=1, keepdims=True)
        u = dot_t(x, wts[i, :, 0].reshape(width, d_model))
        v = dot_t(x, wts[i, :, 1].reshape(width, d_model))
        c = math.sqrt(2.0 / math.pi)
        cdf = 0.5 * (1.0 + jnp.tanh(c * (u + 0.044715 * (u * u * u))))
        a = jnp.where(gate >= 0.0, u * cdf * v, 0.0).astype(jnp.bfloat16)
        for n in range(d_model // ncol):
            cols = pl.ds(n * ncol, ncol)
            o = jnp.dot(a, wts[i, :, 2, :, cols].reshape(width, ncol), preferred_element_type=jnp.float32)
            acc[k, at, cols] += gate * o

    six = 6 * nblk

    def triple(r, q, sets):
        w = q // (2 * nblk)
        i = 3 * r + w + (1 - w) * 2 * py
        work(i, sets + (q // nblk) % 2, q % nblk)

    def run(m0, m1, blocks, block, actions=(), more=True):
        span = m1 - m0

        @pl.loop(0, span)
        def _(j):
            exchange(m0 + j, more)
            for slot, action in actions:
                pl.when(j == slot - m0)(action)

            @pl.loop((blocks * j + span - 1) // span, (blocks * (j + 1) + span - 1) // span)
            def _(q):
                block(q)

    def at_slot(r, j):
        return r * slots + j

    run(at_slot(1, 0), at_slot(2, 0), six, lambda q: triple(0, q, 0), [(at_slot(1, 4), lambda: partner_slices(0))])

    row_copy(2, cross).wait_recv()
    gate_copy(2, cross).wait_recv()
    row_copy(3, sib).start()
    gate_copy(3, sib).start()
    spread_gates(2)

    def far_rows():
        row_copy(3, sib).wait_recv()
        gate_copy(3, sib).wait_recv()
        spread_gates(3)

    run(at_slot(2, 0), at_slot(3, 0), 2 * six, lambda q: triple(1 - q // six, q % six, 2 * (q // six)),
        [(at_slot(2, 2), lambda: partner_slices(1)), (at_slot(2, 3), far_rows)])
    run(at_slot(3, 0), at_slot(4, 0), 2 * six, lambda q: triple(1 + q // six, q % six, 2), [(at_slot(3, 5), lambda: partner_slices(2))])
    early = six // 2
    run(at_slot(4, 0), at_slot(4, 2), early, lambda q: triple(2, q, 0))
    partner_slices(3)
    rest = excl - 9

    @pl.loop(0, 2 * nblk)
    def _(c):
        pl.when(c % nblk == 0)(lambda: exchange(at_slot(4, 2) + c // nblk))

        @pl.loop(0, rest)
        def _(q):
            work(9 + q, 3 - c // nblk, c % nblk)

        @pl.when(c < nblk)
        def _():
            sum_copy(3, fold_out, fold_ss, fold_rs, c, sib).start()

        @pl.when(c >= nblk)
        def _():
            at = pl.ds((c - nblk) * blk, blk)
            sum_copy(3, fold_out, fold_ss, fold_rs, c - nblk, sib).wait_recv()
            bring = pltpu.make_async_copy(fold_out.at[at], tmp, load_sem.at[9])
            bring.start()
            bring.wait()
            acc[2, at, :] += tmp[...]
            sum_copy(2, cross_out, cross_ss, cross_rs, c - nblk, cross).start()

    run(at_slot(4, 4), at_slot(5, 0), six - early, lambda q: triple(2, early + q, 0))
    run(at_slot(5, 0), at_slot(6, 0), six + early, lambda q: triple(3 + q // six, q % six, 0))
    run(at_slot(6, 0), at_slot(7, 0), six + early, lambda q: triple(4 + (q + early) // six, (q + early) % six, 0),
        [(at_slot(6, 0), lambda: partner_slices(4)), (at_slot(6, 5), lambda: partner_slices(5))], more=False)

    last = rounds - 1
    tail = 4 * nblk

    @pl.loop(0, tail)
    def _(q):
        triple(last, q, 0)

    partner_slices(last)

    @pl.loop(0, 2 * nblk)
    def _(q):
        work(3 * last + 2 - 2 * py, 1 - q // nblk, q % nblk)
        pl.when((q >= 1) & (q <= nblk))(lambda: sum_copy(1, part_out, part_ss, part_rs, q - 1, sib).start())

    own = pltpu.make_async_copy(acc.at[0], own_out, load_sem.at[9])
    own.start()

    @pl.loop(0, count)
    def _(m):
        up_copy(m, 1).wait_send()
        dn_copy(m, 1).wait_send()
        y_copy(m, 2 * py).wait_send()

    for k, where in ((1, sib), (2, cross), (3, sib)):
        row_copy(k, where).wait_send()
        gate_copy(k, where).wait_send()
    for c in range(nblk):
        sum_copy(3, fold_out, fold_ss, fold_rs, c, sib).wait_send()
        sum_copy(2, cross_out, cross_ss, cross_rs, c, cross).wait()
        sum_copy(1, part_out, part_ss, part_rs, c, sib).wait()
    own.wait()


def solution(mesh):
    side = math.isqrt(mesh.shape['dp'])
    chips = mesh.shape['wg'] // 2

    def local_block(hidden, choice, pre_scale, w_router, w_gelu, w_linear, w_down, post_scale):
        tok, d_model = hidden.shape
        experts, _, shard = w_gelu.shape
        blk = min(512, tok // 2)
        nblk = tok // blk
        excl = exclusive_experts(experts)
        held = experts - excl
        count = (held // 3) * (chips - 1)
        sums = jax.ShapeDtypeStruct((tok, d_model), jnp.float32)
        dma = pltpu.SemaphoreType.DMA
        flops = 2 * 2 * tok * experts * 3 * (chips * shard) * d_model
        own, part, cross, _ = pl.pallas_call(
            functools.partial(moe_kernel, side, chips, blk, excl),
            out_shape=(sums,) * 4,
            in_specs=[
                pl.BlockSpec(memory_space=pl.ANY),
                pl.BlockSpec(memory_space=pltpu.VMEM),
                pl.BlockSpec(memory_space=pltpu.VMEM),
                pl.BlockSpec(memory_space=pltpu.VMEM),
                pl.BlockSpec(memory_space=pl.ANY),
                pl.BlockSpec(memory_space=pl.ANY),
                pl.BlockSpec(memory_space=pl.ANY),
            ],
            out_specs=(pl.BlockSpec(memory_space=pl.ANY),) * 4,
            scratch_shapes=[
                pltpu.VMEM((held, chips, 3, shard, d_model), jnp.bfloat16),
                pltpu.VMEM((4, tok, d_model), jnp.bfloat16),
                pltpu.VMEM((4, tok, d_model), jnp.float32),
                pltpu.VMEM((4, experts, tok), jnp.float32),
                pltpu.VMEM((4, tok, experts), jnp.float32),
                pltpu.VMEM((blk, d_model), jnp.float32),
                dma((count,)), dma((count,)), dma((count,)), dma((count,)), dma((count,)), dma((count,)),
                dma((10,)),
                dma((3,)), dma((3,)), dma((3,)), dma((3,)),
                dma((nblk,)), dma((nblk,)), dma((nblk,)), dma((nblk,)), dma((nblk,)), dma((nblk,)),
            ],
            compiler_params=pltpu.CompilerParams(collective_id=0, has_side_effects=True, vmem_limit_bytes=VMEM_BYTES),
            cost_estimate=pl.CostEstimate(flops=flops, bytes_accessed=8 * experts * chips * shard * d_model, transcendentals=0),
        )(hidden, choice.T, pre_scale.reshape(1, d_model), w_router.T, jnp.swapaxes(w_gelu, 1, 2), jnp.swapaxes(w_linear, 1, 2), w_down)
        mixed = own + part + cross
        scaled = mixed * lax.rsqrt(jnp.mean(mixed * mixed, axis=-1, keepdims=True) + EPS) * post_scale
        return (hidden.astype(jnp.float32) + scaled).astype(jnp.bfloat16)

    row_spec = P(('dp', 'wg'), None)
    weight_in = P(None, None, 'wg')
    return jax.shard_map(local_block, mesh=mesh, in_specs=(row_spec, row_spec, P(), P(), weight_in, weight_in, P(None, 'wg', None), P()), out_specs=row_spec, check_vma=False)
```

```python
import functools
import math

import jax
import jax.numpy as jnp
from jax import lax
from jax.experimental import pallas as pl
from jax.experimental.pallas import tpu as pltpu
from jax.sharding import PartitionSpec as P

EPS = 1e-5
MESH = pl.DeviceIdType.MESH
SUB = 256
VMEM_BYTES = 67_043_328
OUT = 2 << 20


def dot_t(lhs, rhs):
    return lax.dot_general(lhs, rhs, (((1,), (1,)), ((), ())), preferred_element_type=jnp.float32)


def exclusive_experts(experts):
    count = experts * 11 // 32
    while (experts - count) % 3:
        count -= 1
    return count


def moe_kernel(side, chips, excl, hid_ref, choice_ref, pre_ref, post_ref, router_ref, wg_ref, wl_ref, wd_ref, out_ref,
               wts, rows, acc, gate_t, gates, tmp, up_ss, up_rs, dn_ss, dn_rs, y_ss, y_rs, load_sem, row_ss, row_rs, gate_ss, gate_rs,
               fold_ss, fold_rs, cross_ss, cross_rs, part_ss, part_rs, freed, credit):
    tok, d_model = hid_ref.shape
    held, _, _, shard, _ = wts.shape
    experts = held + excl
    width = chips * shard
    slots = chips - 1
    rounds = held // 3
    count = rounds * slots
    ncol = min(256, d_model)
    chunks = 4
    chunk = tok // chunks
    sub = min(SUB, tok)

    dp, wg = lax.axis_index('dp'), lax.axis_index('wg')
    z, core = wg // 2, wg % 2
    gx, gy = dp // side, dp % side
    px, py = gx % 2, gy % 2
    up = (dp, ((z + 1) % chips) * 2 + core)
    down = (dp, ((z + chips - 1) % chips) * 2 + core)
    sib = (dp, wg + 1 - 2 * core)
    cross = (dp + side * (1 - 2 * px), wg)
    along = (dp + 1 - 2 * py, wg)

    def remote(src, dst, ss, rs, where):
        return pltpu.make_async_remote_copy(src_ref=src, dst_ref=dst, send_sem=ss, recv_sem=rs, device_id=where, device_id_type=MESH)

    def slice_copy(i, chip, ss, rs, m, where):
        ref = wts.at[i, chip]
        return remote(ref, ref, ss.at[m], rs.at[m], where)

    def up_copy(m, back):
        r, j = m // slots, m % slots
        odd, s = j % 2, j // 2 + 1
        i = 3 * r + (1 - odd) * 2 * py + odd
        return slice_copy(i, (z - s + back + chips) % chips, up_ss, up_rs, m, up)

    def dn_copy(m, back):
        r, j = m // slots, m % slots
        odd, s = j % 2, j // 2 + 1
        i = 3 * r + odd * 2 * py + (1 - odd)
        return slice_copy(i, (z + s - back) % chips, dn_ss, dn_rs, m, down)

    def y_copy(m, i):
        r, j = m // slots, m % slots
        odd, s = j % 2, j // 2 + 1
        return slice_copy(3 * r + i, (z + (2 * odd - 1) * s + chips) % chips, y_ss, y_rs, m, along)

    def exchange(m, more=True):
        up_copy(m, 0).wait_recv()
        if more is True:
            up_copy(m + 2, 1).start()
        else:
            pl.when(m + 2 < count)(lambda: up_copy(m + 2, 1).start())
        dn_copy(m, 0).wait_recv()
        if more is True:
            dn_copy(m + 2, 1).start()
        else:
            pl.when(m + 2 < count)(lambda: dn_copy(m + 2, 1).start())
        y_copy(m, 2 * py).start()

    def partner_slices(r):
        @pl.loop(0, slots)
        def _(k):
            y_copy(r * slots + k, 2 - 2 * py).wait_recv()

    def row_copy(k, where):
        return remote(rows.at[0] if k < 3 else rows.at[2], rows.at[k], row_ss.at[k - 1], row_rs.at[k - 1], where)

    def gate_copy(k, where):
        return remote(gate_t.at[0] if k < 3 else gate_t.at[2], gate_t.at[k], gate_ss.at[k - 1], gate_rs.at[k - 1], where)

    def part_of(c):
        return pl.ds(pl.multiple_of(c * chunk, chunk), chunk)

    def fold_copy(c):
        return remote(acc.at[3, part_of(c)], tmp.at[c % 2], fold_ss.at[c], fold_rs.at[c], sib)

    def cross_copy(c):
        return remote(acc.at[2, part_of(c)], tmp.at[(c + 2) % 3], cross_ss.at[c], cross_rs.at[c], cross)

    def free(sem, where):
        pl.semaphore_signal(sem, inc=1, device_id=where, device_id_type=MESH)

    def last_copy(c):
        at = part_of(c)
        return remote(acc.at[1, at], acc.at[3, at], part_ss.at[c], part_rs.at[c], sib)

    loads = []
    for n, (src0, dst0, size) in enumerate(((px * excl, 0, 3), (px * excl + 3, 3, excl - 3), (2 * excl, excl, held - excl))):
        for k, src in enumerate((wg_ref, wl_ref, wd_ref)):
            loads.append(pltpu.make_async_copy(src.at[pl.ds(src0, size)], wts.at[pl.ds(dst0, size), z, k], load_sem.at[3 * n + k]))
    hid_load = pltpu.make_async_copy(hid_ref, rows.at[0], load_sem.at[9])
    for load in loads[:3] + [hid_load] + loads[3:]:
        load.start()

    barrier = pltpu.get_barrier_semaphore()
    for peer in (up, down, sib, cross, along):
        pl.semaphore_signal(barrier, inc=1, device_id=peer, device_id_type=MESH)
    pl.semaphore_wait(barrier, 5)

    for load in loads[:3]:
        load.wait()
    for m in range(2):
        up_copy(m, 1).start()
        dn_copy(m, 1).start()

    hid_load.wait()
    nrm = min(128, chunk)

    @pl.loop(0, tok // nrm)
    def _(i):
        at = pl.ds(pl.multiple_of(i * nrm, nrm), nrm)
        values = rows[0, at, :].astype(jnp.float32)
        scale = lax.rsqrt(jnp.mean(values * values, axis=-1, keepdims=True) + EPS)
        rows[0, at, :] = (values * scale * pre_ref[...]).astype(jnp.bfloat16)

    for load in loads[3:]:
        load.wait()

    rtr = min(256, tok)

    @pl.loop(0, tok // rtr)
    def _(i):
        at = pl.ds(pl.multiple_of(i * rtr, rtr), rtr)
        logits = dot_t(router_ref[...], rows[0, at, :])
        shifted = jnp.exp(logits - jnp.max(logits, axis=0, keepdims=True))
        probs = shifted / jnp.sum(shifted, axis=0, keepdims=True)
        expert_ids = lax.broadcasted_iota(jnp.int32, (experts, rtr), 0)
        picks = choice_ref[:, at]
        chosen = expert_ids == picks[0:1, :]
        for j in range(1, picks.shape[0]):
            chosen = chosen | (expert_ids == picks[j:j + 1, :])
        gate_t[0, :, at] = jnp.where(chosen, probs, -1.0)

    @pl.loop(0, 4 * tok // nrm)
    def _(i):
        at = pl.ds(pl.multiple_of((i // 4) * nrm, nrm), nrm)
        acc[i % 4, at, :] = jnp.zeros((nrm, d_model), jnp.float32)

    for k, where in ((2, cross), (1, sib)):
        gate_copy(k, where).start()
        row_copy(k, where).start()

    def spread_gates(k):
        gates[:, k * experts:(k + 1) * experts] = gate_t[k].T

    spread_gates(0)

    @pl.loop(0, slots)
    def _(j):
        exchange(j)

    row_copy(1, sib).wait_recv()
    gate_copy(1, sib).wait_recv()
    spread_gates(1)

    def work(i, k, starts, size):
        e = i + excl * (px + (1 - px) * jnp.minimum(i // excl, 1)) + k * experts
        lane = lax.broadcasted_iota(jnp.int32, (size, 4 * experts), 1)
        c = math.sqrt(2.0 / math.pi)
        acts = []
        for start in starts:
            at = pl.ds(pl.multiple_of(start, size), size)
            x = rows[k, at, :]
            u = dot_t(x, wts[i, :, 0].reshape(width, d_model))
            v = dot_t(x, wts[i, :, 1].reshape(width, d_model))
            gate = jnp.sum(jnp.where(lane == e, gates[at, :], 0.0), axis=1, keepdims=True)
            cdf = 0.5 * (1.0 + jnp.tanh(c * (u + 0.044715 * (u * u * u))))
            acts.append((at, gate, jnp.where(gate >= 0.0, u * cdf * v, 0.0).astype(jnp.bfloat16)))
        for at, gate, a in acts:
            for n in range(d_model // ncol):
                cols = pl.ds(n * ncol, ncol)
                o = jnp.dot(a, wts[i, :, 2, :, cols].reshape(width, ncol), preferred_element_type=jnp.float32)
                acc[k, at, cols] += gate * o

    def unit(i, k):
        work(i, k, [n * sub for n in range(tok // sub)], sub)

    def held_index(r, w):
        return 3 * r + w + (1 - w) * 2 * py

    def triple(r, q, sets):
        unit(held_index(r, q // 2), sets + q % 2)

    def run(m0, m1, units, one, actions=(), more=True):
        span = m1 - m0

        @pl.loop(0, span)
        def _(j):
            exchange(m0 + j, more)
            for slot, action in actions:
                pl.when(j == slot)(action)

            @pl.loop((units * j + span - 1) // span, (units * (j + 1) + span - 1) // span)
            def _(q):
                one(q)

    run(slots, 2 * slots, 6, lambda q: triple(0, q, 0), [(4, lambda: partner_slices(0))])

    row_copy(2, cross).wait_recv()
    gate_copy(2, cross).wait_recv()
    row_copy(3, sib).start()
    gate_copy(3, sib).start()
    spread_gates(2)

    def far_rows():
        row_copy(3, sib).wait_recv()
        gate_copy(3, sib).wait_recv()
        spread_gates(3)

    run(2 * slots, 3 * slots, 12, lambda q: triple(1 - q // 6, q % 6, 2 * (q // 6)), [(2, lambda: partner_slices(1)), (4, far_rows)])
    run(3 * slots, 4 * slots - 1, 12, lambda q: triple(1 + q // 6, q % 6, 2), [(5, lambda: partner_slices(2))])
    m = 4 * slots - 1
    exchange(m)

    pl.loop(0, 2)(lambda q: unit(excl - 1, 3 - q))
    exchange(m + 1)
    partner_slices(3)

    def late(k, c):
        work(excl - 2, k, [c * chunk], chunk)

    def fold_in(c, slot):
        fold_copy(c).wait_recv()
        acc[2, part_of(c), :] += tmp[slot]

    @pl.loop(0, 2)
    def _(c):
        late(3, c)
        fold_copy(c).start()
        late(2, c)

    exchange(m + 2)

    @pl.loop(0, 2)
    def _(c):
        late(3, 2 + c)
        late(2, 2 + c)
        fold_in(c, c)
        free(freed.at[c], sib)
        pl.when(c == 0)(lambda: cross_copy(0).start())

    for c in range(2):
        pl.semaphore_wait(freed.at[c], 1)
        fold_copy(2 + c).start()
    exchange(m + 3)
    for c in range(2):
        fold_in(2 + c, c)
        free(credit.at[c], cross)
    for c in range(2):
        pl.semaphore_wait(credit.at[c], 1)
        cross_copy(1 + c).start()
    pl.loop(0, chunks)(lambda c: fold_copy(c).wait_send())
    free(freed.at[2], sib)

    def first_sums():
        cross_copy(0).wait_recv()
        acc[0, part_of(0), :] += tmp[2]
        free(credit.at[2], cross)

    def last_sums():
        pl.semaphore_wait(credit.at[2], 1)
        cross_copy(3).start()

    run(m + 4, 5 * slots, 6, lambda q: triple(2, q, 0))
    row_copy(3, sib).wait_send()
    hid_again = pltpu.make_async_copy(hid_ref, rows.at[3], load_sem.at[9])
    hid_again.start()
    run(5 * slots, 6 * slots, 12, lambda q: triple(3 + q // 6, q % 6, 0), [(4, first_sums), (5, lambda: partner_slices(4)), (6, last_sums)])
    run(6 * slots, 7 * slots - 1, 6, lambda q: triple(5, q, 0), [(4, lambda: partner_slices(5))], more=False)
    exchange(count - 1, more=None)

    last = rounds - 1
    pl.loop(0, 3)(lambda q: unit(held_index(last, q % 2), 1 - q // 2))
    partner_slices(last)
    pl.semaphore_wait(freed.at[2], 1)

    @pl.loop(0, chunks)
    def _(c):
        work(held_index(last, 2), 1, [c * chunk], chunk)
        last_copy(c).start()

    pl.loop(1, 3)(lambda q: unit(held_index(last, q), 0))

    @pl.loop(0, count)
    def _(m):
        up_copy(m, 1).wait_send()
        dn_copy(m, 1).wait_send()
        y_copy(m, 2 * py).wait_send()

    for k, where in ((1, sib), (2, cross)):
        row_copy(k, where).wait_send()
    for k, where in ((1, sib), (2, cross), (3, sib)):
        gate_copy(k, where).wait_send()
    hid_again.wait()

    for c in range(chunks):
        last_copy(c).wait()
        cross_copy(c).wait_send()
        if c:
            cross_copy(c).wait_recv()

        @pl.loop(0, chunk // nrm)
        def _(i):
            at = pl.ds(pl.multiple_of(c * chunk + i * nrm, nrm), nrm)
            mixed = acc[0, at, :] + acc[3, at, :]
            if c:
                mixed += tmp[(c + 2) % 3, pl.ds(pl.multiple_of(i * nrm, nrm), nrm), :]
            scale = lax.rsqrt(jnp.mean(mixed * mixed, axis=-1, keepdims=True) + EPS)
            out_ref[at, :] = (rows[3, at, :].astype(jnp.float32) + mixed * scale * post_ref[...]).astype(jnp.bfloat16)


def write_kernel(src_ref, dst_ref, sem):
    write = pltpu.make_async_copy(src_ref, dst_ref, sem)
    write.start()
    write.wait()


def solution(mesh):
    side = math.isqrt(mesh.shape['dp'])
    chips = mesh.shape['wg'] // 2

    def local_block(hidden, choice, pre_scale, w_router, w_gelu, w_linear, w_down, post_scale):
        tok, d_model = hidden.shape
        experts, _, shard = w_gelu.shape
        excl = exclusive_experts(experts)
        held = experts - excl
        count = (held // 3) * (chips - 1)
        dma = pltpu.SemaphoreType.DMA
        vmem = pl.BlockSpec(memory_space=pltpu.VMEM)
        any_space = pl.BlockSpec(memory_space=pl.ANY)
        flops = 2 * 2 * tok * experts * 3 * (chips * shard) * d_model
        out = pl.pallas_call(
            functools.partial(moe_kernel, side, chips, excl),
            out_shape=pltpu.VMEM((tok, d_model), jnp.bfloat16),
            in_specs=[any_space, vmem, vmem, vmem, vmem, any_space, any_space, any_space],
            out_specs=vmem,
            scratch_shapes=[
                pltpu.VMEM((held, chips, 3, shard, d_model), jnp.bfloat16),
                pltpu.VMEM((4, tok, d_model), jnp.bfloat16),
                pltpu.VMEM((4, tok, d_model), jnp.float32),
                pltpu.VMEM((4, experts, tok), jnp.float32),
                pltpu.VMEM((tok, 4 * experts), jnp.float32),
                pltpu.VMEM((3, tok // 4, d_model), jnp.float32),
                dma((count,)), dma((count,)), dma((count,)), dma((count,)), dma((count,)), dma((count,)),
                dma((10,)),
                dma((3,)), dma((3,)), dma((3,)), dma((3,)),
                dma((4,)), dma((4,)), dma((4,)), dma((4,)), dma((4,)), dma((4,)),
                pltpu.SemaphoreType.REGULAR((3,)), pltpu.SemaphoreType.REGULAR((3,)),
            ],
            compiler_params=pltpu.CompilerParams(collective_id=0, has_side_effects=True, vmem_limit_bytes=VMEM_BYTES - OUT),
            cost_estimate=pl.CostEstimate(flops=flops, bytes_accessed=8 * experts * chips * shard * d_model, transcendentals=0),
        )(hidden, choice.T, pre_scale.reshape(1, d_model), post_scale.reshape(1, d_model), w_router.T, jnp.swapaxes(w_gelu, 1, 2), jnp.swapaxes(w_linear, 1, 2), w_down)

        return pl.pallas_call(
            write_kernel,
            out_shape=jax.ShapeDtypeStruct((tok, d_model), jnp.bfloat16),
            in_specs=[vmem],
            out_specs=any_space,
            scratch_shapes=[dma(())],
        )(pltpu.with_memory_space_constraint(out, pltpu.VMEM))

    row_spec = P(('dp', 'wg'), None)
    weight_in = P(None, None, 'wg')
    return jax.shard_map(local_block, mesh=mesh, in_specs=(row_spec, row_spec, P(), P(), weight_in, weight_in, P(None, 'wg', None), P()), out_specs=row_spec, check_vma=False)
```

```python
import functools
import math

import jax
import jax.numpy as jnp
from jax import lax
from jax.experimental import pallas as pl
from jax.experimental.pallas import tpu as pltpu
from jax.sharding import PartitionSpec as P

EPS = 1e-5
MESH = pl.DeviceIdType.MESH
SUB = 256
VMEM_BYTES = 67_043_328
OUT = 2 << 20


def dot_t(lhs, rhs):
    return lax.dot_general(lhs, rhs, (((1,), (1,)), ((), ())), preferred_element_type=jnp.float32)


def exclusive_experts(experts):
    count = experts * 11 // 32
    while (experts - count) % 3:
        count -= 1
    return count


def moe_kernel(side, chips, excl, hid_ref, choice_ref, pre_ref, post_ref, router_ref, wg_ref, wl_ref, wd_ref, out_ref,
               wts, rows, acc, gate_t, gates, tmp, up_ss, up_rs, dn_ss, dn_rs, y_ss, y_rs, load_sem, row_ss, row_rs, gate_ss, gate_rs,
               fold_ss, fold_rs, cross_ss, cross_rs, part_ss, part_rs, freed, credit):
    tok, d_model = hid_ref.shape
    held, _, _, shard, _ = wts.shape
    experts = held + excl
    width = chips * shard
    slots = chips - 1
    rounds = held // 3
    count = rounds * slots
    ncol = min(256, d_model)
    chunks = 4
    chunk = tok // chunks
    sub = min(SUB, tok)

    dp, wg = lax.axis_index('dp'), lax.axis_index('wg')
    z, core = wg // 2, wg % 2
    gx, gy = dp // side, dp % side
    px, py = gx % 2, gy % 2
    up = (dp, ((z + 1) % chips) * 2 + core)
    down = (dp, ((z + chips - 1) % chips) * 2 + core)
    sib = (dp, wg + 1 - 2 * core)
    cross = (dp + side * (1 - 2 * px), wg)
    along = (dp + 1 - 2 * py, wg)

    def remote(src, dst, ss, rs, where):
        return pltpu.make_async_remote_copy(src_ref=src, dst_ref=dst, send_sem=ss, recv_sem=rs, device_id=where, device_id_type=MESH)

    def slice_copy(i, chip, ss, rs, m, where):
        ref = wts.at[i, chip]
        return remote(ref, ref, ss.at[m], rs.at[m], where)

    def up_copy(m, back):
        r, j = m // slots, m % slots
        odd, s = j % 2, j // 2 + 1
        i = 3 * r + (1 - odd) * 2 * py + odd
        return slice_copy(i, (z - s + back + chips) % chips, up_ss, up_rs, m, up)

    def dn_copy(m, back):
        r, j = m // slots, m % slots
        odd, s = j % 2, j // 2 + 1
        i = 3 * r + odd * 2 * py + (1 - odd)
        return slice_copy(i, (z + s - back) % chips, dn_ss, dn_rs, m, down)

    def y_copy(m, i):
        r, j = m // slots, m % slots
        odd, s = j % 2, j // 2 + 1
        return slice_copy(3 * r + i, (z + (2 * odd - 1) * s + chips) % chips, y_ss, y_rs, m, along)

    def exchange(m, more=True, along_y=True):
        up_copy(m, 0).wait_recv()
        if more is True:
            up_copy(m + 2, 1).start()
        else:
            pl.when(m + 2 < count)(lambda: up_copy(m + 2, 1).start())
        dn_copy(m, 0).wait_recv()
        if more is True:
            dn_copy(m + 2, 1).start()
        else:
            pl.when(m + 2 < count)(lambda: dn_copy(m + 2, 1).start())
        if along_y:
            y_copy(m, 2 * py).start()

    def partner_slices(r, first=0, end=slots):
        @pl.loop(first, end)
        def _(k):
            y_copy(r * slots + k, 2 - 2 * py).wait_recv()

    def far_copy(back):
        return slice_copy(3 * (rounds - 1) + 2 - 2 * py, (z - chips // 2 + back + chips) % chips, up_ss, up_rs, count, up)

    def row_copy(k, where):
        return remote(rows.at[0] if k < 3 else rows.at[2], rows.at[k], row_ss.at[k - 1], row_rs.at[k - 1], where)

    def gate_copy(k, where):
        return remote(gate_t.at[0] if k < 3 else gate_t.at[2], gate_t.at[k], gate_ss.at[k - 1], gate_rs.at[k - 1], where)

    def part_of(c):
        return pl.ds(pl.multiple_of(c * chunk, chunk), chunk)

    def fold_copy(c):
        return remote(acc.at[3, part_of(c)], tmp.at[c % 2], fold_ss.at[c], fold_rs.at[c], sib)

    def cross_copy(c):
        return remote(acc.at[2, part_of(c)], tmp.at[(c + 2) % 3], cross_ss.at[c], cross_rs.at[c], cross)

    def free(sem, where):
        pl.semaphore_signal(sem, inc=1, device_id=where, device_id_type=MESH)

    def last_copy(c):
        at = part_of(c)
        return remote(acc.at[1, at], acc.at[3, at], part_ss.at[c], part_rs.at[c], sib)

    loads = []
    for n, (src0, dst0, size) in enumerate(((px * excl, 0, 3), (px * excl + 3, 3, excl - 3), (2 * excl, excl, held - excl))):
        for k, src in enumerate((wg_ref, wl_ref, wd_ref)):
            loads.append(pltpu.make_async_copy(src.at[pl.ds(src0, size)], wts.at[pl.ds(dst0, size), z, k], load_sem.at[3 * n + k]))
    hid_load = pltpu.make_async_copy(hid_ref, rows.at[0], load_sem.at[9])
    for load in loads[:3] + [hid_load] + loads[3:]:
        load.start()

    barrier = pltpu.get_barrier_semaphore()
    for peer in (up, down, sib, cross, along):
        pl.semaphore_signal(barrier, inc=1, device_id=peer, device_id_type=MESH)
    pl.semaphore_wait(barrier, 5)

    for load in loads[:3]:
        load.wait()
    for m in range(2):
        up_copy(m, 1).start()
        dn_copy(m, 1).start()

    hid_load.wait()
    nrm = min(128, chunk)

    @pl.loop(0, tok // nrm)
    def _(i):
        at = pl.ds(pl.multiple_of(i * nrm, nrm), nrm)
        values = rows[0, at, :].astype(jnp.float32)
        scale = lax.rsqrt(jnp.mean(values * values, axis=-1, keepdims=True) + EPS)
        rows[0, at, :] = (values * scale * pre_ref[...]).astype(jnp.bfloat16)

    for load in loads[3:]:
        load.wait()

    rtr = min(256, tok)

    @pl.loop(0, tok // rtr)
    def _(i):
        at = pl.ds(pl.multiple_of(i * rtr, rtr), rtr)
        logits = dot_t(router_ref[...], rows[0, at, :])
        shifted = jnp.exp(logits - jnp.max(logits, axis=0, keepdims=True))
        probs = shifted / jnp.sum(shifted, axis=0, keepdims=True)
        expert_ids = lax.broadcasted_iota(jnp.int32, (experts, rtr), 0)
        picks = choice_ref[:, at]
        chosen = expert_ids == picks[0:1, :]
        for j in range(1, picks.shape[0]):
            chosen = chosen | (expert_ids == picks[j:j + 1, :])
        gate_t[0, :, at] = jnp.where(chosen, probs, -1.0)

    @pl.loop(0, 4 * tok // nrm)
    def _(i):
        at = pl.ds(pl.multiple_of((i // 4) * nrm, nrm), nrm)
        acc[i % 4, at, :] = jnp.zeros((nrm, d_model), jnp.float32)

    for k, where in ((2, cross), (1, sib)):
        gate_copy(k, where).start()
        row_copy(k, where).start()

    def spread_gates(k):
        gates[:, k * experts:(k + 1) * experts] = gate_t[k].T

    spread_gates(0)

    @pl.loop(0, slots)
    def _(j):
        exchange(j)

    row_copy(1, sib).wait_recv()
    gate_copy(1, sib).wait_recv()
    spread_gates(1)

    def work(i, k, starts, size):
        e = i + excl * (px + (1 - px) * jnp.minimum(i // excl, 1)) + k * experts
        lane = lax.broadcasted_iota(jnp.int32, (size, 4 * experts), 1)
        c = math.sqrt(2.0 / math.pi)
        acts = []
        for start in starts:
            at = pl.ds(pl.multiple_of(start, size), size)
            x = rows[k, at, :]
            u = dot_t(x, wts[i, :, 0].reshape(width, d_model))
            v = dot_t(x, wts[i, :, 1].reshape(width, d_model))
            gate = jnp.sum(jnp.where(lane == e, gates[at, :], 0.0), axis=1, keepdims=True)
            cdf = 0.5 * (1.0 + jnp.tanh(c * (u + 0.044715 * (u * u * u))))
            acts.append((at, gate, jnp.where(gate >= 0.0, u * cdf * v, 0.0).astype(jnp.bfloat16)))
        for at, gate, a in acts:
            for n in range(d_model // ncol):
                cols = pl.ds(n * ncol, ncol)
                o = jnp.dot(a, wts[i, :, 2, :, cols].reshape(width, ncol), preferred_element_type=jnp.float32)
                acc[k, at, cols] += gate * o

    def unit(i, k):
        work(i, k, [n * sub for n in range(tok // sub)], sub)

    def held_index(r, w):
        return 3 * r + w + (1 - w) * 2 * py

    def triple(r, q, sets):
        unit(held_index(r, q // 2), sets + q % 2)

    def run(m0, m1, units, one, actions=(), more=True):
        span = m1 - m0

        @pl.loop(0, span)
        def _(j):
            exchange(m0 + j, more)
            for slot, action in actions:
                pl.when(j == slot)(action)

            @pl.loop((units * j + span - 1) // span, (units * (j + 1) + span - 1) // span)
            def _(q):
                one(q)

    run(slots, 2 * slots, 6, lambda q: triple(0, q, 0), [(4, lambda: partner_slices(0))])

    row_copy(2, cross).wait_recv()
    gate_copy(2, cross).wait_recv()
    row_copy(3, sib).start()
    gate_copy(3, sib).start()
    spread_gates(2)

    def far_rows():
        row_copy(3, sib).wait_recv()
        gate_copy(3, sib).wait_recv()
        spread_gates(3)

    run(2 * slots, 3 * slots, 12, lambda q: triple(1 - q // 6, q % 6, 2 * (q // 6)), [(2, lambda: partner_slices(1)), (4, far_rows)])
    run(3 * slots, 4 * slots - 1, 12, lambda q: triple(1 + q // 6, q % 6, 2), [(5, lambda: partner_slices(2))])
    m = 4 * slots - 1
    exchange(m)

    pl.loop(0, 2)(lambda q: unit(excl - 1, 3 - q))
    exchange(m + 1)
    partner_slices(3)

    def late(k, c):
        work(excl - 2, k, [c * chunk], chunk)

    def fold_in(c, slot):
        fold_copy(c).wait_recv()
        acc[2, part_of(c), :] += tmp[slot]

    @pl.loop(0, 2)
    def _(c):
        late(3, c)
        fold_copy(c).start()
        late(2, c)

    exchange(m + 2)

    @pl.loop(0, 2)
    def _(c):
        fold_in(c, c)
        free(freed.at[c], sib)
        pl.when(c == 0)(lambda: cross_copy(0).start())
        late(3, 2 + c)
        late(2, 2 + c)

    for c in range(2):
        pl.semaphore_wait(freed.at[c], 1)
        fold_copy(2 + c).start()
    exchange(m + 3)
    for c in range(2):
        fold_in(2 + c, c)
        free(credit.at[c], cross)
    for c in range(2):
        pl.semaphore_wait(credit.at[c], 1)
        cross_copy(1 + c).start()
    pl.loop(0, chunks)(lambda c: fold_copy(c).wait_send())
    free(freed.at[2], sib)

    def first_sums():
        cross_copy(0).wait_recv()
        acc[0, part_of(0), :] += tmp[2]
        free(credit.at[2], cross)

    def last_sums():
        pl.semaphore_wait(credit.at[2], 1)
        cross_copy(3).start()

    run(m + 4, 5 * slots, 6, lambda q: triple(2, q, 0))
    row_copy(3, sib).wait_send()
    hid_again = pltpu.make_async_copy(hid_ref, rows.at[3], load_sem.at[9])
    hid_again.start()
    run(5 * slots, 6 * slots, 12, lambda q: triple(3 + q // 6, q % 6, 0), [(4, first_sums), (5, lambda: partner_slices(4)), (6, last_sums)])
    run(6 * slots, 7 * slots - 1, 6, lambda q: triple(5, q, 0), [(4, lambda: partner_slices(5))], more=False)
    last = rounds - 1
    partner_slices(last, 0, slots - 2)
    far_copy(1).start()
    exchange(count - 1, more=None, along_y=False)

    pl.loop(0, 2)(lambda q: unit(held_index(last, q), 1))
    partner_slices(last, slots - 2, slots - 1)
    far_copy(0).wait_recv()
    pl.semaphore_wait(freed.at[2], 1)

    @pl.loop(0, chunks)
    def _(c):
        work(held_index(last, 2), 1, [c * chunk], chunk)
        last_copy(c).start()

    pl.loop(0, 3)(lambda q: unit(held_index(last, q), 0))

    @pl.loop(0, count)
    def _(m):
        up_copy(m, 1).wait_send()
        dn_copy(m, 1).wait_send()
        pl.when(m < count - 1)(lambda: y_copy(m, 2 * py).wait_send())

    far_copy(1).wait_send()

    for k, where in ((1, sib), (2, cross)):
        row_copy(k, where).wait_send()
    for k, where in ((1, sib), (2, cross), (3, sib)):
        gate_copy(k, where).wait_send()
    hid_again.wait()

    for c in range(chunks):
        last_copy(c).wait()
        cross_copy(c).wait_send()
        if c:
            cross_copy(c).wait_recv()

        @pl.loop(0, chunk // nrm)
        def _(i):
            at = pl.ds(pl.multiple_of(c * chunk + i * nrm, nrm), nrm)
            mixed = acc[0, at, :] + acc[3, at, :]
            if c:
                mixed += tmp[(c + 2) % 3, pl.ds(pl.multiple_of(i * nrm, nrm), nrm), :]
            scale = lax.rsqrt(jnp.mean(mixed * mixed, axis=-1, keepdims=True) + EPS)
            out_ref[at, :] = (rows[3, at, :].astype(jnp.float32) + mixed * scale * post_ref[...]).astype(jnp.bfloat16)


def write_kernel(src_ref, dst_ref, sem):
    write = pltpu.make_async_copy(src_ref, dst_ref, sem)
    write.start()
    write.wait()


def solution(mesh):
    side = math.isqrt(mesh.shape['dp'])
    chips = mesh.shape['wg'] // 2

    def local_block(hidden, choice, pre_scale, w_router, w_gelu, w_linear, w_down, post_scale):
        tok, d_model = hidden.shape
        experts, _, shard = w_gelu.shape
        excl = exclusive_experts(experts)
        held = experts - excl
        count = (held // 3) * (chips - 1)
        dma = pltpu.SemaphoreType.DMA
        vmem = pl.BlockSpec(memory_space=pltpu.VMEM)
        any_space = pl.BlockSpec(memory_space=pl.ANY)
        flops = 2 * 2 * tok * experts * 3 * (chips * shard) * d_model
        out = pl.pallas_call(
            functools.partial(moe_kernel, side, chips, excl),
            out_shape=pltpu.VMEM((tok, d_model), jnp.bfloat16),
            in_specs=[any_space, vmem, vmem, vmem, vmem, any_space, any_space, any_space],
            out_specs=vmem,
            scratch_shapes=[
                pltpu.VMEM((held, chips, 3, shard, d_model), jnp.bfloat16),
                pltpu.VMEM((4, tok, d_model), jnp.bfloat16),
                pltpu.VMEM((4, tok, d_model), jnp.float32),
                pltpu.VMEM((4, experts, tok), jnp.float32),
                pltpu.VMEM((tok, 4 * experts), jnp.float32),
                pltpu.VMEM((3, tok // 4, d_model), jnp.float32),
                dma((count + 1,)), dma((count + 1,)), dma((count,)), dma((count,)), dma((count,)), dma((count,)),
                dma((10,)),
                dma((3,)), dma((3,)), dma((3,)), dma((3,)),
                dma((4,)), dma((4,)), dma((4,)), dma((4,)), dma((4,)), dma((4,)),
                pltpu.SemaphoreType.REGULAR((3,)), pltpu.SemaphoreType.REGULAR((3,)),
            ],
            compiler_params=pltpu.CompilerParams(collective_id=0, has_side_effects=True, vmem_limit_bytes=VMEM_BYTES - OUT),
            cost_estimate=pl.CostEstimate(flops=flops, bytes_accessed=8 * experts * chips * shard * d_model, transcendentals=0),
        )(hidden, choice.T, pre_scale.reshape(1, d_model), post_scale.reshape(1, d_model), w_router.T, jnp.swapaxes(w_gelu, 1, 2), jnp.swapaxes(w_linear, 1, 2), w_down)

        return pl.pallas_call(
            write_kernel,
            out_shape=jax.ShapeDtypeStruct((tok, d_model), jnp.bfloat16),
            in_specs=[vmem],
            out_specs=any_space,
            scratch_shapes=[dma(())],
        )(pltpu.with_memory_space_constraint(out, pltpu.VMEM))

    row_spec = P(('dp', 'wg'), None)
    weight_in = P(None, None, 'wg')
    return jax.shard_map(local_block, mesh=mesh, in_specs=(row_spec, row_spec, P(), P(), weight_in, weight_in, P(None, 'wg', None), P()), out_specs=row_spec, check_vma=False)
```

```python
import functools
import math

import jax
import jax.numpy as jnp
from jax import lax
from jax.experimental import pallas as pl
from jax.experimental.pallas import tpu as pltpu
from jax.sharding import PartitionSpec as P

EPS = 1e-5
MESH = pl.DeviceIdType.MESH
SUB = 256
VMEM_BYTES = 67_043_328
OUT = 2 << 20


def dot_t(lhs, rhs):
    return lax.dot_general(lhs, rhs, (((1,), (1,)), ((), ())), preferred_element_type=jnp.float32)


def exclusive_experts(experts):
    count = experts * 11 // 32
    while (experts - count) % 3:
        count -= 1
    return count


def moe_kernel(side, chips, excl, hid_ref, choice_ref, pre_ref, post_ref, router_ref, wg_ref, wl_ref, wd_ref, out_ref,
               wts, rows, acc, gate_t, gates, tmp, up_ss, up_rs, dn_ss, dn_rs, y_ss, y_rs, load_sem, row_ss, row_rs, gate_ss, gate_rs,
               fold_ss, fold_rs, cross_ss, cross_rs, part_ss, part_rs, freed, credit):
    tok, d_model = hid_ref.shape
    held, _, _, shard, _ = wts.shape
    experts = held + excl
    width = chips * shard
    slots = chips - 1
    rounds = held // 3
    count = rounds * slots
    ncol = min(256, d_model)
    chunks = 4
    chunk = tok // chunks
    sub = min(SUB, tok)

    dp, wg = lax.axis_index('dp'), lax.axis_index('wg')
    z, core = wg // 2, wg % 2
    gx, gy = dp // side, dp % side
    px, py = gx % 2, gy % 2
    up = (dp, ((z + 1) % chips) * 2 + core)
    down = (dp, ((z + chips - 1) % chips) * 2 + core)
    sib = (dp, wg + 1 - 2 * core)
    cross = (dp + side * (1 - 2 * px), wg)
    along = (dp + 1 - 2 * py, wg)

    def remote(src, dst, ss, rs, where):
        return pltpu.make_async_remote_copy(src_ref=src, dst_ref=dst, send_sem=ss, recv_sem=rs, device_id=where, device_id_type=MESH)

    def slice_copy(i, chip, ss, rs, m, where):
        ref = wts.at[i, chip]
        return remote(ref, ref, ss.at[m], rs.at[m], where)

    def up_copy(m, back):
        r, j = m // slots, m % slots
        odd, s = j % 2, j // 2 + 1
        i = 3 * r + (1 - odd) * 2 * py + odd
        return slice_copy(i, (z - s + back + chips) % chips, up_ss, up_rs, m, up)

    def dn_copy(m, back):
        r, j = m // slots, m % slots
        odd, s = j % 2, j // 2 + 1
        i = 3 * r + odd * 2 * py + (1 - odd)
        return slice_copy(i, (z + s - back) % chips, dn_ss, dn_rs, m, down)

    def y_copy(m, i):
        r, j = m // slots, m % slots
        odd, s = j % 2, j // 2 + 1
        return slice_copy(3 * r + i, (z + (2 * odd - 1) * s + chips) % chips, y_ss, y_rs, m, along)

    def exchange(m, more=True, along_y=True):
        up_copy(m, 0).wait_recv()
        if more is True:
            up_copy(m + 2, 1).start()
        else:
            pl.when(m + 2 < count)(lambda: up_copy(m + 2, 1).start())
        dn_copy(m, 0).wait_recv()
        if more is True:
            dn_copy(m + 2, 1).start()
        else:
            pl.when(m + 2 < count)(lambda: dn_copy(m + 2, 1).start())
        if along_y:
            y_copy(m, 2 * py).start()

    def partner_slices(r, first=0, end=slots):
        @pl.loop(first, end)
        def _(k):
            y_copy(r * slots + k, 2 - 2 * py).wait_recv()

    def far_copy(back):
        return slice_copy(3 * (rounds - 1) + 2 - 2 * py, (z - chips // 2 + back + chips) % chips, up_ss, up_rs, count, up)

    def row_copy(k, where):
        return remote(rows.at[0] if k < 3 else rows.at[2], rows.at[k], row_ss.at[k - 1], row_rs.at[k - 1], where)

    def gate_copy(k, where):
        return remote(gate_t.at[0] if k < 3 else gate_t.at[2], gate_t.at[k], gate_ss.at[k - 1], gate_rs.at[k - 1], where)

    def part_of(c):
        return pl.ds(pl.multiple_of(c * chunk, chunk), chunk)

    h = chunk // 2
    pieces = ((0, h, 0, 0, 2, 0), (h, h, 0, h, 2, h), (chunk, chunk, 1, 0, 0, 0), (2 * chunk, chunk, 0, 0, 1, 0), (3 * chunk, chunk, 1, 0, 2, 0))

    def fold_copy(n):
        at, size, slot, row, _, _ = pieces[n]
        return remote(acc.at[3, pl.ds(at, size)], tmp.at[slot, pl.ds(row, size)], fold_ss.at[n], fold_rs.at[n], sib)

    def cross_copy(n):
        at, size, _, _, slot, row = pieces[n]
        return remote(acc.at[2, pl.ds(at, size)], tmp.at[slot, pl.ds(row, size)], cross_ss.at[n], cross_rs.at[n], cross)

    def free(sem, where):
        pl.semaphore_signal(sem, inc=1, device_id=where, device_id_type=MESH)

    def last_copy(c):
        at = part_of(c)
        return remote(acc.at[1, at], acc.at[3, at], part_ss.at[c], part_rs.at[c], sib)

    loads = []
    for n, (src0, dst0, size) in enumerate(((px * excl, 0, 3), (px * excl + 3, 3, excl - 3), (2 * excl, excl, held - excl))):
        for k, src in enumerate((wg_ref, wl_ref, wd_ref)):
            loads.append(pltpu.make_async_copy(src.at[pl.ds(src0, size)], wts.at[pl.ds(dst0, size), z, k], load_sem.at[3 * n + k]))
    hid_load = pltpu.make_async_copy(hid_ref, rows.at[0], load_sem.at[9])
    for load in loads[:3]:
        load.start()

    barrier = pltpu.get_barrier_semaphore()
    for peer in (up, down, sib, cross, along):
        pl.semaphore_signal(barrier, inc=1, device_id=peer, device_id_type=MESH)
    pl.semaphore_wait(barrier, 5)

    for load in loads[:3]:
        load.wait()
    for m in range(2):
        up_copy(m, 1).start()
        dn_copy(m, 1).start()

    router_load = pltpu.make_async_copy(router_ref, out_ref.at[pl.ds(0, experts)], load_sem.at[10])
    for load in [hid_load, router_load] + loads[3:]:
        load.start()
    nrm = min(128, chunk)

    @pl.loop(0, 4 * tok // nrm)
    def _(i):
        at = pl.ds(pl.multiple_of((i // 4) * nrm, nrm), nrm)
        acc[i % 4, at, :] = jnp.zeros((nrm, d_model), jnp.float32)

    hid_load.wait()

    @pl.loop(0, tok // nrm)
    def _(i):
        at = pl.ds(pl.multiple_of(i * nrm, nrm), nrm)
        values = rows[0, at, :].astype(jnp.float32)
        scale = lax.rsqrt(jnp.mean(values * values, axis=-1, keepdims=True) + EPS)
        rows[0, at, :] = (values * scale * pre_ref[...]).astype(jnp.bfloat16)

    for load in loads[3:]:
        load.wait()

    router_load.wait()
    rtr = min(256, tok)

    @pl.loop(0, tok // rtr)
    def _(i):
        at = pl.ds(pl.multiple_of(i * rtr, rtr), rtr)
        logits = dot_t(out_ref[pl.ds(0, experts), :], rows[0, at, :])
        shifted = jnp.exp(logits - jnp.max(logits, axis=0, keepdims=True))
        probs = shifted / jnp.sum(shifted, axis=0, keepdims=True)
        expert_ids = lax.broadcasted_iota(jnp.int32, (experts, rtr), 0)
        picks = choice_ref[:, at]
        chosen = expert_ids == picks[0:1, :]
        for j in range(1, picks.shape[0]):
            chosen = chosen | (expert_ids == picks[j:j + 1, :])
        gate_t[0, :, at] = jnp.where(chosen, probs, -1.0)

    for k, where in ((2, cross), (1, sib)):
        gate_copy(k, where).start()
        row_copy(k, where).start()

    def spread_gates(k):
        gates[:, k * experts:(k + 1) * experts] = gate_t[k].T

    spread_gates(0)

    @pl.loop(0, slots)
    def _(j):
        exchange(j)

    row_copy(1, sib).wait_recv()
    gate_copy(1, sib).wait_recv()
    spread_gates(1)

    def work(i, k, starts, size):
        e = i + excl * (px + (1 - px) * jnp.minimum(i // excl, 1)) + k * experts
        lane = lax.broadcasted_iota(jnp.int32, (size, 4 * experts), 1)
        c = math.sqrt(2.0 / math.pi)
        acts = []
        for start in starts:
            at = pl.ds(pl.multiple_of(start, size), size)
            x = rows[k, at, :]
            u = dot_t(x, wts[i, :, 0].reshape(width, d_model))
            v = dot_t(x, wts[i, :, 1].reshape(width, d_model))
            gate = jnp.sum(jnp.where(lane == e, gates[at, :], 0.0), axis=1, keepdims=True)
            cdf = 0.5 * (1.0 + jnp.tanh(c * (u + 0.044715 * (u * u * u))))
            acts.append((at, gate, jnp.where(gate >= 0.0, u * cdf * v, 0.0).astype(jnp.bfloat16)))
        for at, gate, a in acts:
            for n in range(d_model // ncol):
                cols = pl.ds(n * ncol, ncol)
                o = jnp.dot(a, wts[i, :, 2, :, cols].reshape(width, ncol), preferred_element_type=jnp.float32)
                acc[k, at, cols] += gate * o

    def unit(i, k):
        work(i, k, [n * sub for n in range(tok // sub)], sub)

    def held_index(r, w):
        return 3 * r + w + (1 - w) * 2 * py

    def triple(r, q, sets):
        unit(held_index(r, q // 2), sets + q % 2)

    def run(m0, m1, units, one, actions=(), more=True):
        span = m1 - m0

        @pl.loop(0, span)
        def _(j):
            exchange(m0 + j, more)
            for slot, action in actions:
                pl.when(j == slot)(action)

            @pl.loop((units * j + span - 1) // span, (units * (j + 1) + span - 1) // span)
            def _(q):
                one(q)

    run(slots, 2 * slots, 6, lambda q: triple(0, q, 0), [(4, lambda: partner_slices(0))])

    row_copy(2, cross).wait_recv()
    gate_copy(2, cross).wait_recv()
    row_copy(3, sib).start()
    gate_copy(3, sib).start()
    spread_gates(2)

    def far_rows():
        row_copy(3, sib).wait_recv()
        gate_copy(3, sib).wait_recv()
        spread_gates(3)

    run(2 * slots, 3 * slots, 12, lambda q: triple(1 - q // 6, q % 6, 2 * (q // 6)), [(2, lambda: partner_slices(1)), (4, far_rows)])
    run(3 * slots, 4 * slots - 1, 12, lambda q: triple(1 + q // 6, q % 6, 2), [(5, lambda: partner_slices(2))])
    m = 4 * slots - 1
    exchange(m)

    pl.loop(0, 2)(lambda q: unit(excl - 1, 3 - q))
    exchange(m + 1)
    partner_slices(3)

    def late(k, start, size):
        work(excl - 2, k, [start], size)

    def fold_in(n):
        at, size, slot, row, _, _ = pieces[n]
        fold_copy(n).wait_recv()

        @pl.loop(0, size // h)
        def _(i):
            acc[2, pl.ds(pl.multiple_of(at + i * h, h), h), :] += tmp[slot, pl.ds(pl.multiple_of(row + i * h, h), h), :]

    @pl.loop(0, 2)
    def _(n):
        late(3, n * h, h)
        part = pl.ds(pl.multiple_of(n * h, h), h)
        remote(acc.at[3, part], tmp.at[0, part], fold_ss.at[n], fold_rs.at[n], sib).start()
        late(2, n * h, h)

    late(3, *pieces[2][:2])
    fold_copy(2).start()
    fold_in(0)
    cross_copy(0).start()
    exchange(m + 2)
    late(2, *pieces[2][:2])
    fold_in(1)
    cross_copy(1).start()
    free(freed.at[0], sib)
    fold_in(2)
    free(freed.at[1], sib)

    @pl.loop(2, chunks)
    def _(c):
        late(3, c * chunk, chunk)
        late(2, c * chunk, chunk)

    for n in range(2):
        pl.semaphore_wait(freed.at[n], 1)
        fold_copy(3 + n).start()
    exchange(m + 3)
    for n in range(2):
        fold_in(3 + n)
        free(credit.at[n], cross)
    for n in range(2):
        pl.semaphore_wait(credit.at[n], 1)
        cross_copy(2 + n).start()
    for n in range(len(pieces)):
        fold_copy(n).wait_send()
    free(freed.at[2], sib)

    def first_sums():
        for n in range(2):
            cross_copy(n).wait_recv()

        @pl.loop(0, 2)
        def _(i):
            part = pl.ds(pl.multiple_of(i * h, h), h)
            acc[0, part, :] += tmp[2, part, :]

        free(credit.at[2], cross)

    def last_sums():
        pl.semaphore_wait(credit.at[2], 1)
        cross_copy(4).start()

    run(m + 4, 5 * slots, 6, lambda q: triple(2, q, 0))
    row_copy(3, sib).wait_send()
    hid_again = pltpu.make_async_copy(hid_ref, rows.at[3], load_sem.at[9])
    hid_again.start()
    run(5 * slots, 6 * slots, 12, lambda q: triple(3 + q // 6, q % 6, 0), [(4, first_sums), (5, lambda: partner_slices(4)), (6, last_sums)])
    run(6 * slots, 7 * slots - 1, 6, lambda q: triple(5, q, 0), [(4, lambda: partner_slices(5))], more=False)
    last = rounds - 1
    partner_slices(last, 0, slots - 2)
    far_copy(1).start()
    exchange(count - 1, more=None, along_y=False)

    pl.loop(0, 2)(lambda q: unit(held_index(last, q), 1))
    partner_slices(last, slots - 2, slots - 1)
    far_copy(0).wait_recv()
    pl.semaphore_wait(freed.at[2], 1)

    @pl.loop(0, 2)
    def _(q):
        work(held_index(last, 2), 1, [(2 * q + n) * chunk for n in range(2)], chunk)
        last_copy(2 * q).start()
        last_copy(2 * q + 1).start()

    pl.loop(0, 3)(lambda q: unit(held_index(last, q), 0))

    @pl.loop(0, count)
    def _(m):
        up_copy(m, 1).wait_send()
        dn_copy(m, 1).wait_send()
        pl.when(m < count - 1)(lambda: y_copy(m, 2 * py).wait_send())

    far_copy(1).wait_send()

    for k, where in ((1, sib), (2, cross)):
        row_copy(k, where).wait_send()
    for k, where in ((1, sib), (2, cross), (3, sib)):
        gate_copy(k, where).wait_send()
    hid_again.wait()

    for n in range(len(pieces)):
        cross_copy(n).wait_send()
    for c in range(chunks):
        last_copy(c).wait()
        if c:
            cross_copy(c + 1).wait_recv()

        @pl.loop(0, chunk // nrm)
        def _(i):
            at = pl.ds(pl.multiple_of(c * chunk + i * nrm, nrm), nrm)
            mixed = acc[0, at, :] + acc[3, at, :]
            if c:
                mixed += tmp[(c + 2) % 3, pl.ds(pl.multiple_of(i * nrm, nrm), nrm), :]
            scale = lax.rsqrt(jnp.mean(mixed * mixed, axis=-1, keepdims=True) + EPS)
            out_ref[at, :] = (rows[3, at, :].astype(jnp.float32) + mixed * scale * post_ref[...]).astype(jnp.bfloat16)


def write_kernel(src_ref, dst_ref, sem):
    write = pltpu.make_async_copy(src_ref, dst_ref, sem)
    write.start()
    write.wait()


def solution(mesh):
    side = math.isqrt(mesh.shape['dp'])
    chips = mesh.shape['wg'] // 2

    def local_block(hidden, choice, pre_scale, w_router, w_gelu, w_linear, w_down, post_scale):
        tok, d_model = hidden.shape
        experts, _, shard = w_gelu.shape
        excl = exclusive_experts(experts)
        held = experts - excl
        count = (held // 3) * (chips - 1)
        dma = pltpu.SemaphoreType.DMA
        vmem = pl.BlockSpec(memory_space=pltpu.VMEM)
        any_space = pl.BlockSpec(memory_space=pl.ANY)
        flops = 2 * 2 * tok * experts * 3 * (chips * shard) * d_model
        out = pl.pallas_call(
            functools.partial(moe_kernel, side, chips, excl),
            out_shape=pltpu.VMEM((tok, d_model), jnp.bfloat16),
            in_specs=[any_space, vmem, vmem, vmem, any_space, any_space, any_space, any_space],
            out_specs=vmem,
            scratch_shapes=[
                pltpu.VMEM((held, chips, 3, shard, d_model), jnp.bfloat16),
                pltpu.VMEM((4, tok, d_model), jnp.bfloat16),
                pltpu.VMEM((4, tok, d_model), jnp.float32),
                pltpu.VMEM((4, experts, tok), jnp.float32),
                pltpu.VMEM((tok, 4 * experts), jnp.float32),
                pltpu.VMEM((3, tok // 4, d_model), jnp.float32),
                dma((count + 1,)), dma((count + 1,)), dma((count,)), dma((count,)), dma((count,)), dma((count,)),
                dma((11,)),
                dma((3,)), dma((3,)), dma((3,)), dma((3,)),
                dma((5,)), dma((5,)), dma((5,)), dma((5,)), dma((4,)), dma((4,)),
                pltpu.SemaphoreType.REGULAR((3,)), pltpu.SemaphoreType.REGULAR((3,)),
            ],
            compiler_params=pltpu.CompilerParams(collective_id=0, has_side_effects=True, vmem_limit_bytes=VMEM_BYTES - OUT),
            cost_estimate=pl.CostEstimate(flops=flops, bytes_accessed=8 * experts * chips * shard * d_model, transcendentals=0),
        )(hidden, choice.T, pre_scale.reshape(1, d_model), post_scale.reshape(1, d_model), w_router.T, jnp.swapaxes(w_gelu, 1, 2), jnp.swapaxes(w_linear, 1, 2), w_down)

        return pl.pallas_call(
            write_kernel,
            out_shape=jax.ShapeDtypeStruct((tok, d_model), jnp.bfloat16),
            in_specs=[vmem],
            out_specs=any_space,
            scratch_shapes=[dma(())],
        )(pltpu.with_memory_space_constraint(out, pltpu.VMEM))

    row_spec = P(('dp', 'wg'), None)
    weight_in = P(None, None, 'wg')
    return jax.shard_map(local_block, mesh=mesh, in_specs=(row_spec, row_spec, P(), P(), weight_in, weight_in, P(None, 'wg', None), P()), out_specs=row_spec, check_vma=False)
```

```python
import functools
import math

import jax
import jax.numpy as jnp
from jax import lax
from jax.experimental import pallas as pl
from jax.experimental.pallas import tpu as pltpu
from jax.sharding import PartitionSpec as P

EPS = 1e-5
MESH = pl.DeviceIdType.MESH
SUB = 256
VMEM_BYTES = 67_043_328
OUT = 2 << 20


def dot_t(lhs, rhs):
    return lax.dot_general(lhs, rhs, (((1,), (1,)), ((), ())), preferred_element_type=jnp.float32)


def exclusive_experts(experts):
    count = experts * 11 // 32
    while (experts - count) % 3:
        count -= 1
    return count


def moe_kernel(side, chips, excl, hid_ref, choice_ref, pre_ref, post_ref, router_ref, wg_ref, wl_ref, wd_ref, out_ref,
               wts, rows, acc, gate_t, gates, tmp, up_ss, up_rs, dn_ss, dn_rs, y_ss, y_rs, load_sem, row_ss, row_rs, gate_ss, gate_rs,
               fold_ss, fold_rs, cross_ss, cross_rs, part_ss, part_rs, freed, credit):
    tok, d_model = hid_ref.shape
    held, _, _, shard, _ = wts.shape
    experts = held + excl
    width = chips * shard
    slots = chips - 1
    rounds = held // 3
    count = rounds * slots
    ncol = min(256, d_model)
    chunks = 4
    chunk = tok // chunks
    sub = min(SUB, tok)

    dp, wg = lax.axis_index('dp'), lax.axis_index('wg')
    z, core = wg // 2, wg % 2
    gx, gy = dp // side, dp % side
    px, py = gx % 2, gy % 2
    up = (dp, ((z + 1) % chips) * 2 + core)
    down = (dp, ((z + chips - 1) % chips) * 2 + core)
    sib = (dp, wg + 1 - 2 * core)
    cross = (dp + side * (1 - 2 * px), wg)
    along = (dp + 1 - 2 * py, wg)

    def remote(src, dst, ss, rs, where):
        return pltpu.make_async_remote_copy(src_ref=src, dst_ref=dst, send_sem=ss, recv_sem=rs, device_id=where, device_id_type=MESH)

    def slice_copy(i, chip, ss, rs, m, where):
        ref = wts.at[i, chip]
        return remote(ref, ref, ss.at[m], rs.at[m], where)

    def up_copy(m, back):
        r, j = m // slots, m % slots
        odd, s = j % 2, j // 2 + 1
        i = 3 * r + (1 - odd) * 2 * py + odd
        return slice_copy(i, (z - s + back + chips) % chips, up_ss, up_rs, m, up)

    def dn_copy(m, back):
        r, j = m // slots, m % slots
        odd, s = j % 2, j // 2 + 1
        i = 3 * r + odd * 2 * py + (1 - odd)
        return slice_copy(i, (z + s - back) % chips, dn_ss, dn_rs, m, down)

    def y_copy(m, i):
        r, j = m // slots, m % slots
        odd, s = j % 2, j // 2 + 1
        return slice_copy(3 * r + i, (z + (2 * odd - 1) * s + chips) % chips, y_ss, y_rs, m, along)

    def exchange(m, more=True, along_y=True):
        up_copy(m, 0).wait_recv()
        if more is True:
            up_copy(m + 2, 1).start()
        else:
            pl.when(m + 2 < count)(lambda: up_copy(m + 2, 1).start())
        dn_copy(m, 0).wait_recv()
        if more is True:
            dn_copy(m + 2, 1).start()
        else:
            pl.when(m + 2 < count)(lambda: dn_copy(m + 2, 1).start())
        if along_y:
            y_copy(m, 2 * py).start()

    def partner_slices(r, first=0, end=slots):
        @pl.loop(first, end)
        def _(k):
            y_copy(r * slots + k, 2 - 2 * py).wait_recv()

    def far_copy(back):
        return slice_copy(3 * (rounds - 1) + 2 - 2 * py, (z - chips // 2 + back + chips) % chips, up_ss, up_rs, count, up)

    def row_copy(k, where):
        return remote(rows.at[0] if k < 3 else rows.at[2], rows.at[k], row_ss.at[k - 1], row_rs.at[k - 1], where)

    def gate_copy(k, where):
        return remote(gate_t.at[0] if k < 3 else gate_t.at[2], gate_t.at[k], gate_ss.at[k - 1], gate_rs.at[k - 1], where)

    def part_of(c):
        return pl.ds(pl.multiple_of(c * chunk, chunk), chunk)

    def fold_copy(c):
        return remote(acc.at[3, part_of(c)], tmp.at[c % 2], fold_ss.at[c], fold_rs.at[c], sib)

    def cross_copy(c):
        return remote(acc.at[2, part_of(c)], tmp.at[(c + 2) % 3], cross_ss.at[c], cross_rs.at[c], cross)

    def free(sem, where):
        pl.semaphore_signal(sem, inc=1, device_id=where, device_id_type=MESH)

    def last_copy(c):
        at = part_of(c)
        return remote(acc.at[1, at], acc.at[3, at], part_ss.at[c], part_rs.at[c], sib)

    loads = []
    for n, (src0, dst0, size) in enumerate(((px * excl, 0, 3), (px * excl + 3, 3, excl - 3), (2 * excl, excl, held - excl))):
        for k, src in enumerate((wg_ref, wl_ref, wd_ref)):
            loads.append(pltpu.make_async_copy(src.at[pl.ds(src0, size)], wts.at[pl.ds(dst0, size), z, k], load_sem.at[3 * n + k]))
    hid_load = pltpu.make_async_copy(hid_ref, rows.at[0], load_sem.at[9])
    for load in loads[:3] + [hid_load] + loads[3:]:
        load.start()

    barrier = pltpu.get_barrier_semaphore()
    for peer in (up, down, sib, cross, along):
        pl.semaphore_signal(barrier, inc=1, device_id=peer, device_id_type=MESH)
    pl.semaphore_wait(barrier, 5)

    for load in loads[:3]:
        load.wait()
    for m in range(2):
        up_copy(m, 1).start()
        dn_copy(m, 1).start()

    hid_load.wait()
    nrm = min(128, chunk)

    @pl.loop(0, tok // nrm)
    def _(i):
        at = pl.ds(pl.multiple_of(i * nrm, nrm), nrm)
        values = rows[0, at, :].astype(jnp.float32)
        scale = lax.rsqrt(jnp.mean(values * values, axis=-1, keepdims=True) + EPS)
        rows[0, at, :] = (values * scale * pre_ref[...]).astype(jnp.bfloat16)

    for load in loads[3:]:
        load.wait()

    rtr = min(256, tok)

    @pl.loop(0, tok // rtr)
    def _(i):
        at = pl.ds(pl.multiple_of(i * rtr, rtr), rtr)
        logits = dot_t(router_ref[...], rows[0, at, :])
        shifted = jnp.exp(logits - jnp.max(logits, axis=0, keepdims=True))
        probs = shifted / jnp.sum(shifted, axis=0, keepdims=True)
        expert_ids = lax.broadcasted_iota(jnp.int32, (experts, rtr), 0)
        picks = choice_ref[:, at]
        chosen = expert_ids == picks[0:1, :]
        for j in range(1, picks.shape[0]):
            chosen = chosen | (expert_ids == picks[j:j + 1, :])
        gate_t[0, :, at] = jnp.where(chosen, probs, -1.0)

    @pl.loop(0, 4 * tok // nrm)
    def _(i):
        at = pl.ds(pl.multiple_of((i // 4) * nrm, nrm), nrm)
        acc[i % 4, at, :] = jnp.zeros((nrm, d_model), jnp.float32)

    for k, where in ((2, cross), (1, sib)):
        gate_copy(k, where).start()
        row_copy(k, where).start()

    def spread_gates(k):
        gates[:, k * experts:(k + 1) * experts] = gate_t[k].T

    spread_gates(0)

    @pl.loop(0, slots)
    def _(j):
        exchange(j)

    row_copy(1, sib).wait_recv()
    gate_copy(1, sib).wait_recv()
    spread_gates(1)

    def work(i, k, starts, size):
        e = i + excl * (px + (1 - px) * jnp.minimum(i // excl, 1)) + k * experts
        lane = lax.broadcasted_iota(jnp.int32, (size, 4 * experts), 1)
        c = math.sqrt(2.0 / math.pi)
        acts = []
        for start in starts:
            at = pl.ds(pl.multiple_of(start, size), size)
            x = rows[k, at, :]
            u = dot_t(x, wts[i, :, 0].reshape(width, d_model))
            v = dot_t(x, wts[i, :, 1].reshape(width, d_model))
            gate = jnp.sum(jnp.where(lane == e, gates[at, :], 0.0), axis=1, keepdims=True)
            cdf = 0.5 * (1.0 + jnp.tanh(c * (u + 0.044715 * (u * u * u))))
            acts.append((at, gate, jnp.where(gate >= 0.0, u * cdf * v, 0.0).astype(jnp.bfloat16)))
        for at, gate, a in acts:
            for n in range(d_model // ncol):
                cols = pl.ds(n * ncol, ncol)
                o = jnp.dot(a, wts[i, :, 2, :, cols].reshape(width, ncol), preferred_element_type=jnp.float32)
                acc[k, at, cols] += gate * o

    def unit(i, k):
        work(i, k, [n * sub for n in range(tok // sub)], sub)

    def held_index(r, w):
        return 3 * r + w + (1 - w) * 2 * py

    def triple(r, q, sets):
        unit(held_index(r, q // 2), sets + q % 2)

    def run(m0, m1, units, one, actions=(), more=True):
        span = m1 - m0

        @pl.loop(0, span)
        def _(j):
            exchange(m0 + j, more)
            for slot, action in actions:
                pl.when(j == slot)(action)

            @pl.loop((units * j + span - 1) // span, (units * (j + 1) + span - 1) // span)
            def _(q):
                one(q)

    run(slots, 2 * slots, 6, lambda q: triple(0, q, 0), [(4, lambda: partner_slices(0))])

    row_copy(2, cross).wait_recv()
    gate_copy(2, cross).wait_recv()
    row_copy(3, sib).start()
    gate_copy(3, sib).start()
    spread_gates(2)

    def far_rows():
        row_copy(3, sib).wait_recv()
        gate_copy(3, sib).wait_recv()
        spread_gates(3)

    run(2 * slots, 3 * slots, 12, lambda q: unit(held_index((q % 6) // 3, q % 3), 2 + q // 6), [(2, lambda: partner_slices(1)), (3, far_rows)])
    run(3 * slots, 4 * slots - 1, 6, lambda q: triple(2, q, 2), [(4, lambda: partner_slices(2))])
    m = 4 * slots - 1
    exchange(m)

    pl.loop(0, 2)(lambda q: unit(excl - 1, 3 - q))
    exchange(m + 1)
    partner_slices(3)

    def late(k, c):
        work(excl - 2, k, [c * chunk], chunk)

    def fold_in(c, slot):
        fold_copy(c).wait_recv()
        acc[2, part_of(c), :] += tmp[slot]

    @pl.loop(0, 2)
    def _(c):
        late(3, c)
        fold_copy(c).start()
        late(2, c)

    exchange(m + 2)

    @pl.loop(0, 2)
    def _(c):
        fold_in(c, c)
        free(freed.at[c], sib)
        pl.when(c == 0)(lambda: cross_copy(0).start())
        late(3, 2 + c)
        late(2, 2 + c)

    for c in range(2):
        pl.semaphore_wait(freed.at[c], 1)
        fold_copy(2 + c).start()
    exchange(m + 3)
    for c in range(2):
        fold_in(2 + c, c)
        free(credit.at[c], cross)
    for c in range(2):
        pl.semaphore_wait(credit.at[c], 1)
        cross_copy(1 + c).start()
    pl.loop(0, chunks)(lambda c: fold_copy(c).wait_send())
    free(freed.at[2], sib)

    def first_sums():
        cross_copy(0).wait_recv()
        acc[0, part_of(0), :] += tmp[2]
        free(credit.at[2], cross)

    def last_sums():
        pl.semaphore_wait(credit.at[2], 1)
        cross_copy(3).start()

    def own(q):
        triple(1 + q // 6, q % 6, 0)

    run(m + 4, 5 * slots, 7, own)
    row_copy(3, sib).wait_send()
    hid_again = pltpu.make_async_copy(hid_ref, rows.at[3], load_sem.at[9])
    hid_again.start()
    run(5 * slots, 6 * slots, 13, lambda q: own(7 + q), [(4, first_sums), (6, last_sums)])
    run(6 * slots, 7 * slots - 1, 10, lambda q: own(20 + q), [(0, lambda: partner_slices(4)), (4, lambda: partner_slices(5))], more=False)
    last = rounds - 1
    partner_slices(last, 0, slots - 2)
    far_copy(1).start()
    exchange(count - 1, more=None, along_y=False)

    pl.loop(0, 2)(lambda q: unit(held_index(last, q), 1))
    partner_slices(last, slots - 2, slots - 1)
    far_copy(0).wait_recv()
    pl.semaphore_wait(freed.at[2], 1)

    @pl.loop(0, chunks)
    def _(c):
        work(held_index(last, 2), 1, [c * chunk], chunk)
        last_copy(c).start()

    pl.loop(0, 3)(lambda q: unit(held_index(last, q), 0))

    @pl.loop(0, count)
    def _(m):
        up_copy(m, 1).wait_send()
        dn_copy(m, 1).wait_send()
        pl.when(m < count - 1)(lambda: y_copy(m, 2 * py).wait_send())

    far_copy(1).wait_send()

    for k, where in ((1, sib), (2, cross)):
        row_copy(k, where).wait_send()
    for k, where in ((1, sib), (2, cross), (3, sib)):
        gate_copy(k, where).wait_send()
    hid_again.wait()

    for c in range(chunks):
        last_copy(c).wait()
        cross_copy(c).wait_send()
        if c:
            cross_copy(c).wait_recv()

        @pl.loop(0, chunk // nrm)
        def _(i):
            at = pl.ds(pl.multiple_of(c * chunk + i * nrm, nrm), nrm)
            mixed = acc[0, at, :] + acc[3, at, :]
            if c:
                mixed += tmp[(c + 2) % 3, pl.ds(pl.multiple_of(i * nrm, nrm), nrm), :]
            scale = lax.rsqrt(jnp.mean(mixed * mixed, axis=-1, keepdims=True) + EPS)
            out_ref[at, :] = (rows[3, at, :].astype(jnp.float32) + mixed * scale * post_ref[...]).astype(jnp.bfloat16)


def write_kernel(src_ref, dst_ref, sem):
    write = pltpu.make_async_copy(src_ref, dst_ref, sem)
    write.start()
    write.wait()


def solution(mesh):
    side = math.isqrt(mesh.shape['dp'])
    chips = mesh.shape['wg'] // 2

    def local_block(hidden, choice, pre_scale, w_router, w_gelu, w_linear, w_down, post_scale):
        tok, d_model = hidden.shape
        experts, _, shard = w_gelu.shape
        excl = exclusive_experts(experts)
        held = experts - excl
        count = (held // 3) * (chips - 1)
        dma = pltpu.SemaphoreType.DMA
        vmem = pl.BlockSpec(memory_space=pltpu.VMEM)
        any_space = pl.BlockSpec(memory_space=pl.ANY)
        flops = 2 * 2 * tok * experts * 3 * (chips * shard) * d_model
        out = pl.pallas_call(
            functools.partial(moe_kernel, side, chips, excl),
            out_shape=pltpu.VMEM((tok, d_model), jnp.bfloat16),
            in_specs=[any_space, vmem, vmem, vmem, vmem, any_space, any_space, any_space],
            out_specs=vmem,
            scratch_shapes=[
                pltpu.VMEM((held, chips, 3, shard, d_model), jnp.bfloat16),
                pltpu.VMEM((4, tok, d_model), jnp.bfloat16),
                pltpu.VMEM((4, tok, d_model), jnp.float32),
                pltpu.VMEM((4, experts, tok), jnp.float32),
                pltpu.VMEM((tok, 4 * experts), jnp.float32),
                pltpu.VMEM((3, tok // 4, d_model), jnp.float32),
                dma((count + 1,)), dma((count + 1,)), dma((count,)), dma((count,)), dma((count,)), dma((count,)),
                dma((10,)),
                dma((3,)), dma((3,)), dma((3,)), dma((3,)),
                dma((4,)), dma((4,)), dma((4,)), dma((4,)), dma((4,)), dma((4,)),
                pltpu.SemaphoreType.REGULAR((3,)), pltpu.SemaphoreType.REGULAR((3,)),
            ],
            compiler_params=pltpu.CompilerParams(collective_id=0, has_side_effects=True, vmem_limit_bytes=VMEM_BYTES - OUT),
            cost_estimate=pl.CostEstimate(flops=flops, bytes_accessed=8 * experts * chips * shard * d_model, transcendentals=0),
        )(hidden, choice.T, pre_scale.reshape(1, d_model), post_scale.reshape(1, d_model), w_router.T, jnp.swapaxes(w_gelu, 1, 2), jnp.swapaxes(w_linear, 1, 2), w_down)

        return pl.pallas_call(
            write_kernel,
            out_shape=jax.ShapeDtypeStruct((tok, d_model), jnp.bfloat16),
            in_specs=[vmem],
            out_specs=any_space,
            scratch_shapes=[dma(())],
        )(pltpu.with_memory_space_constraint(out, pltpu.VMEM))

    row_spec = P(('dp', 'wg'), None)
    weight_in = P(None, None, 'wg')
    return jax.shard_map(local_block, mesh=mesh, in_specs=(row_spec, row_spec, P(), P(), weight_in, weight_in, P(None, 'wg', None), P()), out_specs=row_spec, check_vma=False)
```

```python
import functools
import math

import jax
import jax.numpy as jnp
from jax import lax
from jax.experimental import pallas as pl
from jax.experimental.pallas import tpu as pltpu
from jax.sharding import PartitionSpec as P

EPS = 1e-5
MESH = pl.DeviceIdType.MESH
SUB = 256
VMEM_BYTES = 67_043_328
OUT = 2 << 20


def dot_t(lhs, rhs):
    return lax.dot_general(lhs, rhs, (((1,), (1,)), ((), ())), preferred_element_type=jnp.float32)


def exclusive_experts(experts):
    count = experts * 11 // 32
    while (experts - count) % 3:
        count -= 1
    return count


def moe_kernel(side, chips, excl, hid_ref, choice_ref, pre_ref, post_ref, router_ref, wg_ref, wl_ref, wd_ref, out_ref,
               wts, rows, acc, gate_t, gates, tmp, up_ss, up_rs, dn_ss, dn_rs, y_ss, y_rs, load_sem, row_ss, row_rs, gate_ss, gate_rs,
               fold_ss, fold_rs, cross_ss, cross_rs, part_ss, part_rs, freed, credit):
    tok, d_model = hid_ref.shape
    held, _, _, shard, _ = wts.shape
    experts = held + excl
    width = chips * shard
    slots = chips - 1
    rounds = held // 3
    count = rounds * slots
    ncol = min(256, d_model)
    chunks = 4
    chunk = tok // chunks
    sub = min(SUB, tok)

    dp, wg = lax.axis_index('dp'), lax.axis_index('wg')
    z, core = wg // 2, wg % 2
    gx, gy = dp // side, dp % side
    px, py = gx % 2, gy % 2
    up = (dp, ((z + 1) % chips) * 2 + core)
    down = (dp, ((z + chips - 1) % chips) * 2 + core)
    sib = (dp, wg + 1 - 2 * core)
    cross = (dp + side * (1 - 2 * px), wg)
    along = (dp + 1 - 2 * py, wg)

    def remote(src, dst, ss, rs, where):
        return pltpu.make_async_remote_copy(src_ref=src, dst_ref=dst, send_sem=ss, recv_sem=rs, device_id=where, device_id_type=MESH)

    def slice_copy(i, chip, ss, rs, m, where):
        ref = wts.at[i, chip]
        return remote(ref, ref, ss.at[m], rs.at[m], where)

    def up_copy(m, back):
        r, j = m // slots, m % slots
        odd, s = j % 2, j // 2 + 1
        i = 3 * r + (1 - odd) * 2 * py + odd
        return slice_copy(i, (z - s + back + chips) % chips, up_ss, up_rs, m, up)

    def dn_copy(m, back):
        r, j = m // slots, m % slots
        odd, s = j % 2, j // 2 + 1
        i = 3 * r + odd * 2 * py + (1 - odd)
        return slice_copy(i, (z + s - back) % chips, dn_ss, dn_rs, m, down)

    def y_copy(m, i):
        r, j = m // slots, m % slots
        odd, s = j % 2, j // 2 + 1
        return slice_copy(3 * r + i, (z + (2 * odd - 1) * s + chips) % chips, y_ss, y_rs, m, along)

    def exchange(m, more=True, along_y=True):
        up_copy(m, 0).wait_recv()
        if more is True:
            up_copy(m + 2, 1).start()
        else:
            pl.when(m + 2 < count)(lambda: up_copy(m + 2, 1).start())
        dn_copy(m, 0).wait_recv()
        if more is True:
            dn_copy(m + 2, 1).start()
        else:
            pl.when(m + 2 < count)(lambda: dn_copy(m + 2, 1).start())
        if along_y:
            y_copy(m, 2 * py).start()

    def partner_slices(r, first=0, end=slots):
        @pl.loop(first, end)
        def _(k):
            y_copy(r * slots + k, 2 - 2 * py).wait_recv()

    def far_copy(back):
        return slice_copy(3 * (rounds - 1) + 2 - 2 * py, (z - chips // 2 + back + chips) % chips, up_ss, up_rs, count, up)

    def row_copy(k, where):
        return remote(rows.at[0] if k < 3 else rows.at[2], rows.at[k], row_ss.at[k - 1], row_rs.at[k - 1], where)

    def gate_copy(k, where):
        return remote(gate_t.at[0] if k < 3 else gate_t.at[2], gate_t.at[k], gate_ss.at[k - 1], gate_rs.at[k - 1], where)

    def part_of(c):
        return pl.ds(pl.multiple_of(c * chunk, chunk), chunk)

    h = chunk // 2
    pieces = ((0, h, 0, 0, 2, 0), (h, h, 0, h, 2, h), (chunk, chunk, 1, 0, 0, 0), (2 * chunk, chunk, 0, 0, 1, 0), (3 * chunk, chunk, 1, 0, 2, 0))

    def fold_copy(n):
        at, size, slot, row, _, _ = pieces[n]
        return remote(acc.at[3, pl.ds(at, size)], tmp.at[slot, pl.ds(row, size)], fold_ss.at[n], fold_rs.at[n], sib)

    def cross_copy(n):
        at, size, _, _, slot, row = pieces[n]
        return remote(acc.at[2, pl.ds(at, size)], tmp.at[slot, pl.ds(row, size)], cross_ss.at[n], cross_rs.at[n], cross)

    def free(sem, where):
        pl.semaphore_signal(sem, inc=1, device_id=where, device_id_type=MESH)

    def last_copy(c):
        at = part_of(c)
        return remote(acc.at[1, at], acc.at[3, at], part_ss.at[c], part_rs.at[c], sib)

    loads = []
    for n, (src0, dst0, size) in enumerate(((px * excl, 0, 3), (px * excl + 3, 3, excl - 3), (2 * excl, excl, held - excl))):
        for k, src in enumerate((wg_ref, wl_ref, wd_ref)):
            loads.append(pltpu.make_async_copy(src.at[pl.ds(src0, size)], wts.at[pl.ds(dst0, size), z, k], load_sem.at[3 * n + k]))
    hid_load = pltpu.make_async_copy(hid_ref, rows.at[0], load_sem.at[9])
    router_load = pltpu.make_async_copy(router_ref, out_ref.at[pl.ds(0, experts)], load_sem.at[10])
    for load in loads[:3] + [hid_load, router_load] + loads[3:]:
        load.start()

    barrier = pltpu.get_barrier_semaphore()
    for peer in (up, down, sib, cross, along):
        pl.semaphore_signal(barrier, inc=1, device_id=peer, device_id_type=MESH)
    pl.semaphore_wait(barrier, 5)

    for load in loads[:3]:
        load.wait()
    for m in range(2):
        up_copy(m, 1).start()
        dn_copy(m, 1).start()

    nrm = min(128, chunk)

    @pl.loop(0, 4 * tok // nrm)
    def _(i):
        at = pl.ds(pl.multiple_of((i // 4) * nrm, nrm), nrm)
        acc[i % 4, at, :] = jnp.zeros((nrm, d_model), jnp.float32)

    hid_load.wait()

    @pl.loop(0, tok // nrm)
    def _(i):
        at = pl.ds(pl.multiple_of(i * nrm, nrm), nrm)
        values = rows[0, at, :].astype(jnp.float32)
        scale = lax.rsqrt(jnp.mean(values * values, axis=-1, keepdims=True) + EPS)
        rows[0, at, :] = (values * scale * pre_ref[...]).astype(jnp.bfloat16)

    for load in loads[3:]:
        load.wait()

    router_load.wait()
    rtr = min(256, tok)

    @pl.loop(0, tok // rtr)
    def _(i):
        at = pl.ds(pl.multiple_of(i * rtr, rtr), rtr)
        logits = dot_t(out_ref[pl.ds(0, experts), :], rows[0, at, :])
        shifted = jnp.exp(logits - jnp.max(logits, axis=0, keepdims=True))
        probs = shifted / jnp.sum(shifted, axis=0, keepdims=True)
        expert_ids = lax.broadcasted_iota(jnp.int32, (experts, rtr), 0)
        picks = choice_ref[:, at]
        chosen = expert_ids == picks[0:1, :]
        for j in range(1, picks.shape[0]):
            chosen = chosen | (expert_ids == picks[j:j + 1, :])
        gate_t[0, :, at] = jnp.where(chosen, probs, -1.0)

    for k, where in ((2, cross), (1, sib)):
        gate_copy(k, where).start()
        row_copy(k, where).start()

    def spread_gates(k):
        gates[:, k * experts:(k + 1) * experts] = gate_t[k].T

    spread_gates(0)

    @pl.loop(0, slots)
    def _(j):
        exchange(j)

    row_copy(1, sib).wait_recv()
    gate_copy(1, sib).wait_recv()
    spread_gates(1)

    def work(i, k, starts, size):
        e = i + excl * (px + (1 - px) * jnp.minimum(i // excl, 1)) + k * experts
        lane = lax.broadcasted_iota(jnp.int32, (size, 4 * experts), 1)
        c = math.sqrt(2.0 / math.pi)
        acts = []
        for start in starts:
            at = pl.ds(pl.multiple_of(start, size), size)
            x = rows[k, at, :]
            u = dot_t(x, wts[i, :, 0].reshape(width, d_model))
            v = dot_t(x, wts[i, :, 1].reshape(width, d_model))
            gate = jnp.sum(jnp.where(lane == e, gates[at, :], 0.0), axis=1, keepdims=True)
            cdf = 0.5 * (1.0 + jnp.tanh(c * (u + 0.044715 * (u * u * u))))
            acts.append((at, gate, jnp.where(gate >= 0.0, u * cdf * v, 0.0).astype(jnp.bfloat16)))
        for at, gate, a in acts:
            for n in range(d_model // ncol):
                cols = pl.ds(n * ncol, ncol)
                o = jnp.dot(a, wts[i, :, 2, :, cols].reshape(width, ncol), preferred_element_type=jnp.float32)
                acc[k, at, cols] += gate * o

    def unit(i, k):
        work(i, k, [n * sub for n in range(tok // sub)], sub)

    def held_index(r, w):
        return 3 * r + w + (1 - w) * 2 * py

    def triple(r, q, sets):
        unit(held_index(r, q // 2), sets + q % 2)

    def run(m0, m1, units, one, actions=(), more=True):
        span = m1 - m0

        @pl.loop(0, span)
        def _(j):
            exchange(m0 + j, more)
            for slot, action in actions:
                pl.when(j == slot)(action)

            @pl.loop((units * j + span - 1) // span, (units * (j + 1) + span - 1) // span)
            def _(q):
                one(q)

    run(slots, 2 * slots, 6, lambda q: triple(0, q, 0), [(4, lambda: partner_slices(0))])

    row_copy(2, cross).wait_recv()
    gate_copy(2, cross).wait_recv()
    row_copy(3, sib).start()
    gate_copy(3, sib).start()
    spread_gates(2)

    def far_rows():
        row_copy(3, sib).wait_recv()
        gate_copy(3, sib).wait_recv()
        spread_gates(3)

    run(2 * slots, 3 * slots, 12, lambda q: triple(1 - q // 6, q % 6, 2 * (q // 6)), [(2, lambda: partner_slices(1)), (4, far_rows)])
    run(3 * slots, 4 * slots - 1, 12, lambda q: triple(1 + q // 6, q % 6, 2), [(5, lambda: partner_slices(2))])
    m = 4 * slots - 1
    exchange(m)

    pl.loop(0, 2)(lambda q: unit(excl - 1, 3 - q))
    exchange(m + 1)
    partner_slices(3)

    def late(k, start, size):
        work(excl - 2, k, [start], size)

    def fold_in(n):
        at, size, slot, row, _, _ = pieces[n]
        fold_copy(n).wait_recv()

        @pl.loop(0, size // h)
        def _(i):
            acc[2, pl.ds(pl.multiple_of(at + i * h, h), h), :] += tmp[slot, pl.ds(pl.multiple_of(row + i * h, h), h), :]

    @pl.loop(0, 2)
    def _(n):
        late(3, n * h, h)
        part = pl.ds(pl.multiple_of(n * h, h), h)
        remote(acc.at[3, part], tmp.at[0, part], fold_ss.at[n], fold_rs.at[n], sib).start()
        late(2, n * h, h)

    late(3, *pieces[2][:2])
    fold_copy(2).start()
    fold_in(0)
    cross_copy(0).start()
    exchange(m + 2)
    late(2, *pieces[2][:2])
    fold_in(1)
    cross_copy(1).start()
    free(freed.at[0], sib)
    fold_in(2)
    free(freed.at[1], sib)

    exchange(m + 3)

    @pl.loop(2, chunks)
    def _(c):
        late(3, c * chunk, chunk)
        late(2, c * chunk, chunk)

    for n in range(2):
        pl.semaphore_wait(freed.at[n], 1)
        fold_copy(3 + n).start()
    exchange(m + 4)
    for n in range(2):
        fold_in(3 + n)
        free(credit.at[n], cross)
    exchange(m + 5)
    for n in range(2):
        pl.semaphore_wait(credit.at[n], 1)
        cross_copy(2 + n).start()
    for n in range(len(pieces)):
        fold_copy(n).wait_send()
    free(freed.at[2], sib)

    def first_sums():
        for n in range(2):
            cross_copy(n).wait_recv()

        @pl.loop(0, 2)
        def _(i):
            part = pl.ds(pl.multiple_of(i * h, h), h)
            acc[0, part, :] += tmp[2, part, :]

        free(credit.at[2], cross)

    def last_sums():
        pl.semaphore_wait(credit.at[2], 1)
        cross_copy(4).start()

    def own(q):
        triple(2 + q // 6, q % 6, 0)

    run(m + 6, 5 * slots, 3, own)
    row_copy(3, sib).wait_send()
    hid_again = pltpu.make_async_copy(hid_ref, rows.at[3], load_sem.at[9])
    hid_again.start()
    run(5 * slots, 6 * slots, 12, lambda q: own(3 + q), [(4, first_sums), (6, last_sums)])
    run(6 * slots, 7 * slots - 1, 9, lambda q: own(15 + q), [(0, lambda: partner_slices(4)), (4, lambda: partner_slices(5))], more=False)
    last = rounds - 1
    partner_slices(last, 0, slots - 2)
    far_copy(1).start()
    exchange(count - 1, more=None, along_y=False)

    pl.loop(0, 2)(lambda q: unit(held_index(last, q), 1))
    partner_slices(last, slots - 2, slots - 1)
    far_copy(0).wait_recv()
    pl.semaphore_wait(freed.at[2], 1)

    @pl.loop(0, 2)
    def _(q):
        work(held_index(last, 2), 1, [(2 * q + n) * chunk for n in range(2)], chunk)
        last_copy(2 * q).start()
        last_copy(2 * q + 1).start()

    pl.loop(0, 3)(lambda q: unit(held_index(last, q), 0))

    @pl.loop(0, count)
    def _(m):
        up_copy(m, 1).wait_send()
        dn_copy(m, 1).wait_send()
        pl.when(m < count - 1)(lambda: y_copy(m, 2 * py).wait_send())

    far_copy(1).wait_send()

    for k, where in ((1, sib), (2, cross)):
        row_copy(k, where).wait_send()
    for k, where in ((1, sib), (2, cross), (3, sib)):
        gate_copy(k, where).wait_send()
    hid_again.wait()

    for n in range(len(pieces)):
        cross_copy(n).wait_send()
    for c in range(chunks):
        last_copy(c).wait()
        if c:
            cross_copy(c + 1).wait_recv()

        @pl.loop(0, chunk // nrm)
        def _(i):
            at = pl.ds(pl.multiple_of(c * chunk + i * nrm, nrm), nrm)
            mixed = acc[0, at, :] + acc[3, at, :]
            if c:
                mixed += tmp[(c + 2) % 3, pl.ds(pl.multiple_of(i * nrm, nrm), nrm), :]
            scale = lax.rsqrt(jnp.mean(mixed * mixed, axis=-1, keepdims=True) + EPS)
            out_ref[at, :] = (rows[3, at, :].astype(jnp.float32) + mixed * scale * post_ref[...]).astype(jnp.bfloat16)


def write_kernel(src_ref, dst_ref, sem):
    write = pltpu.make_async_copy(src_ref, dst_ref, sem)
    write.start()
    write.wait()


def solution(mesh):
    side = math.isqrt(mesh.shape['dp'])
    chips = mesh.shape['wg'] // 2

    def local_block(hidden, choice, pre_scale, w_router, w_gelu, w_linear, w_down, post_scale):
        tok, d_model = hidden.shape
        experts, _, shard = w_gelu.shape
        excl = exclusive_experts(experts)
        held = experts - excl
        count = (held // 3) * (chips - 1)
        dma = pltpu.SemaphoreType.DMA
        vmem = pl.BlockSpec(memory_space=pltpu.VMEM)
        any_space = pl.BlockSpec(memory_space=pl.ANY)
        flops = 2 * 2 * tok * experts * 3 * (chips * shard) * d_model
        out = pl.pallas_call(
            functools.partial(moe_kernel, side, chips, excl),
            out_shape=pltpu.VMEM((tok, d_model), jnp.bfloat16),
            in_specs=[any_space, vmem, vmem, vmem, any_space, any_space, any_space, any_space],
            out_specs=vmem,
            scratch_shapes=[
                pltpu.VMEM((held, chips, 3, shard, d_model), jnp.bfloat16),
                pltpu.VMEM((4, tok, d_model), jnp.bfloat16),
                pltpu.VMEM((4, tok, d_model), jnp.float32),
                pltpu.VMEM((4, experts, tok), jnp.float32),
                pltpu.VMEM((tok, 4 * experts), jnp.float32),
                pltpu.VMEM((3, tok // 4, d_model), jnp.float32),
                dma((count + 1,)), dma((count + 1,)), dma((count,)), dma((count,)), dma((count,)), dma((count,)),
                dma((11,)),
                dma((3,)), dma((3,)), dma((3,)), dma((3,)),
                dma((5,)), dma((5,)), dma((5,)), dma((5,)), dma((4,)), dma((4,)),
                pltpu.SemaphoreType.REGULAR((3,)), pltpu.SemaphoreType.REGULAR((3,)),
            ],
            compiler_params=pltpu.CompilerParams(collective_id=0, has_side_effects=True, vmem_limit_bytes=VMEM_BYTES - OUT),
            cost_estimate=pl.CostEstimate(flops=flops, bytes_accessed=8 * experts * chips * shard * d_model, transcendentals=0),
        )(hidden, choice.T, pre_scale.reshape(1, d_model), post_scale.reshape(1, d_model), w_router.T, jnp.swapaxes(w_gelu, 1, 2), jnp.swapaxes(w_linear, 1, 2), w_down)

        return pl.pallas_call(
            write_kernel,
            out_shape=jax.ShapeDtypeStruct((tok, d_model), jnp.bfloat16),
            in_specs=[vmem],
            out_specs=any_space,
            scratch_shapes=[dma(())],
        )(pltpu.with_memory_space_constraint(out, pltpu.VMEM))

    row_spec = P(('dp', 'wg'), None)
    weight_in = P(None, None, 'wg')
    return jax.shard_map(local_block, mesh=mesh, in_specs=(row_spec, row_spec, P(), P(), weight_in, weight_in, P(None, 'wg', None), P()), out_specs=row_spec, check_vma=False)
```

```python
import functools
import math

import jax
import jax.numpy as jnp
from jax import lax
from jax.experimental import pallas as pl
from jax.experimental.pallas import tpu as pltpu
from jax.sharding import PartitionSpec as P

EPS = 1e-5
MESH = pl.DeviceIdType.MESH
SUB = 256
VMEM_BYTES = 67_043_328
OUT = 2 << 20


def dot_t(lhs, rhs):
    return lax.dot_general(lhs, rhs, (((1,), (1,)), ((), ())), preferred_element_type=jnp.float32)


def exclusive_experts(experts):
    count = experts * 11 // 32
    while (experts - count) % 3:
        count -= 1
    return count


def moe_kernel(side, chips, excl, hid_ref, choice_ref, pre_ref, post_ref, router_ref, wg_ref, wl_ref, wd_ref, out_ref,
               wts, rows, acc, gate_t, gates, tmp, up_ss, up_rs, dn_ss, dn_rs, y_ss, y_rs, load_sem, row_ss, row_rs, gate_ss, gate_rs,
               fold_ss, fold_rs, cross_ss, cross_rs, part_ss, part_rs, freed, credit):
    tok, d_model = hid_ref.shape
    held, _, _, shard, _ = wts.shape
    experts = held + excl
    width = chips * shard
    slots = chips - 1
    rounds = held // 3
    count = rounds * slots
    ncol = min(256, d_model)
    chunks = 4
    chunk = tok // chunks
    sub = min(SUB, tok)

    dp, wg = lax.axis_index('dp'), lax.axis_index('wg')
    z, core = wg // 2, wg % 2
    gx, gy = dp // side, dp % side
    px, py = gx % 2, gy % 2
    up = (dp, ((z + 1) % chips) * 2 + core)
    down = (dp, ((z + chips - 1) % chips) * 2 + core)
    sib = (dp, wg + 1 - 2 * core)
    cross = (dp + side * (1 - 2 * px), wg)
    along = (dp + 1 - 2 * py, wg)

    def remote(src, dst, ss, rs, where):
        return pltpu.make_async_remote_copy(src_ref=src, dst_ref=dst, send_sem=ss, recv_sem=rs, device_id=where, device_id_type=MESH)

    def slice_copy(i, chip, ss, rs, m, where):
        ref = wts.at[i, chip]
        return remote(ref, ref, ss.at[m], rs.at[m], where)

    def up_copy(m, back):
        r, j = m // slots, m % slots
        odd, s = j % 2, j // 2 + 1
        i = 3 * r + (1 - odd) * 2 * py + odd
        return slice_copy(i, (z - s + back + chips) % chips, up_ss, up_rs, m, up)

    def dn_copy(m, back):
        r, j = m // slots, m % slots
        odd, s = j % 2, j // 2 + 1
        i = 3 * r + odd * 2 * py + (1 - odd)
        return slice_copy(i, (z + s - back) % chips, dn_ss, dn_rs, m, down)

    def y_copy(m, i):
        r, j = m // slots, m % slots
        odd, s = j % 2, j // 2 + 1
        return slice_copy(3 * r + i, (z + (2 * odd - 1) * s + chips) % chips, y_ss, y_rs, m, along)

    def exchange(m, more=True, along_y=True):
        up_copy(m, 0).wait_recv()
        if more is True:
            up_copy(m + 2, 1).start()
        else:
            pl.when(m + 2 < count)(lambda: up_copy(m + 2, 1).start())
        dn_copy(m, 0).wait_recv()
        if more is True:
            dn_copy(m + 2, 1).start()
        else:
            pl.when(m + 2 < count)(lambda: dn_copy(m + 2, 1).start())
        if along_y:
            y_copy(m, 2 * py).start()

    def partner_slices(r, first=0, end=slots):
        @pl.loop(first, end)
        def _(k):
            y_copy(r * slots + k, 2 - 2 * py).wait_recv()

    def far_copy(back):
        return slice_copy(3 * (rounds - 1) + 2 - 2 * py, (z - chips // 2 + back + chips) % chips, up_ss, up_rs, count, up)

    def row_copy(k, where):
        return remote(rows.at[0] if k < 3 else rows.at[2], rows.at[k], row_ss.at[k - 1], row_rs.at[k - 1], where)

    def gate_copy(k, where):
        return remote(gate_t.at[0] if k < 3 else gate_t.at[2], gate_t.at[k], gate_ss.at[k - 1], gate_rs.at[k - 1], where)

    def part_of(c):
        return pl.ds(pl.multiple_of(c * chunk, chunk), chunk)

    h = chunk // 2
    g = h // 2
    pieces = ((0, g, 0, 0, 2, 0), (g, g, 0, g, 2, g), (h, h, 0, h, 2, h), (chunk, chunk, 1, 0, 0, 0), (2 * chunk, chunk, 0, 0, 1, 0), (3 * chunk, chunk, 1, 0, 2, 0))

    def fold_copy(n):
        at, size, slot, row, _, _ = pieces[n]
        return remote(acc.at[3, pl.ds(at, size)], tmp.at[slot, pl.ds(row, size)], fold_ss.at[n], fold_rs.at[n], sib)

    def cross_copy(n):
        at, size, _, _, slot, row = pieces[n]
        return remote(acc.at[2, pl.ds(at, size)], tmp.at[slot, pl.ds(row, size)], cross_ss.at[n], cross_rs.at[n], cross)

    def free(sem, where):
        pl.semaphore_signal(sem, inc=1, device_id=where, device_id_type=MESH)

    def last_copy(c):
        at = part_of(c)
        return remote(acc.at[1, at], acc.at[3, at], part_ss.at[c], part_rs.at[c], sib)

    loads = []
    for n, (src0, dst0, size) in enumerate(((px * excl, 0, 3), (px * excl + 3, 3, excl - 3), (2 * excl, excl, held - excl))):
        for k, src in enumerate((wg_ref, wl_ref, wd_ref)):
            loads.append(pltpu.make_async_copy(src.at[pl.ds(src0, size)], wts.at[pl.ds(dst0, size), z, k], load_sem.at[3 * n + k]))
    hid_load = pltpu.make_async_copy(hid_ref, rows.at[0], load_sem.at[9])
    router_load = pltpu.make_async_copy(router_ref, out_ref.at[pl.ds(0, experts)], load_sem.at[10])
    for load in loads[:3] + [hid_load, router_load] + loads[3:]:
        load.start()

    barrier = pltpu.get_barrier_semaphore()
    for peer in (up, down, sib, cross, along):
        pl.semaphore_signal(barrier, inc=1, device_id=peer, device_id_type=MESH)
    pl.semaphore_wait(barrier, 5)

    for load in loads[:3]:
        load.wait()
    for m in range(2):
        up_copy(m, 1).start()
        dn_copy(m, 1).start()

    nrm = min(128, chunk)

    @pl.loop(0, 4 * tok // nrm)
    def _(i):
        at = pl.ds(pl.multiple_of((i // 4) * nrm, nrm), nrm)
        acc[i % 4, at, :] = jnp.zeros((nrm, d_model), jnp.float32)

    hid_load.wait()

    @pl.loop(0, tok // nrm)
    def _(i):
        at = pl.ds(pl.multiple_of(i * nrm, nrm), nrm)
        values = rows[0, at, :].astype(jnp.float32)
        scale = lax.rsqrt(jnp.mean(values * values, axis=-1, keepdims=True) + EPS)
        rows[0, at, :] = (values * scale * pre_ref[...]).astype(jnp.bfloat16)

    for load in loads[3:]:
        load.wait()

    router_load.wait()
    rtr = min(256, tok)

    @pl.loop(0, tok // rtr)
    def _(i):
        at = pl.ds(pl.multiple_of(i * rtr, rtr), rtr)
        logits = dot_t(out_ref[pl.ds(0, experts), :], rows[0, at, :])
        shifted = jnp.exp(logits - jnp.max(logits, axis=0, keepdims=True))
        probs = shifted / jnp.sum(shifted, axis=0, keepdims=True)
        expert_ids = lax.broadcasted_iota(jnp.int32, (experts, rtr), 0)
        picks = choice_ref[:, at]
        chosen = expert_ids == picks[0:1, :]
        for j in range(1, picks.shape[0]):
            chosen = chosen | (expert_ids == picks[j:j + 1, :])
        gate_t[0, :, at] = jnp.where(chosen, probs, -1.0)

    for k, where in ((2, cross), (1, sib)):
        gate_copy(k, where).start()
        row_copy(k, where).start()

    def spread_gates(k):
        gates[:, k * experts:(k + 1) * experts] = gate_t[k].T

    spread_gates(0)

    @pl.loop(0, slots)
    def _(j):
        exchange(j)

    row_copy(1, sib).wait_recv()
    gate_copy(1, sib).wait_recv()
    spread_gates(1)

    def work(i, k, starts, size):
        e = i + excl * (px + (1 - px) * jnp.minimum(i // excl, 1)) + k * experts
        lane = lax.broadcasted_iota(jnp.int32, (size, 4 * experts), 1)
        c = math.sqrt(2.0 / math.pi)
        acts = []
        for start in starts:
            at = pl.ds(pl.multiple_of(start, size), size)
            x = rows[k, at, :]
            u = dot_t(x, wts[i, :, 0].reshape(width, d_model))
            v = dot_t(x, wts[i, :, 1].reshape(width, d_model))
            gate = jnp.sum(jnp.where(lane == e, gates[at, :], 0.0), axis=1, keepdims=True)
            cdf = 0.5 * (1.0 + jnp.tanh(c * (u + 0.044715 * (u * u * u))))
            acts.append((at, gate, jnp.where(gate >= 0.0, u * cdf * v, 0.0).astype(jnp.bfloat16)))
        for at, gate, a in acts:
            for n in range(d_model // ncol):
                cols = pl.ds(n * ncol, ncol)
                o = jnp.dot(a, wts[i, :, 2, :, cols].reshape(width, ncol), preferred_element_type=jnp.float32)
                acc[k, at, cols] += gate * o

    def unit(i, k):
        work(i, k, [n * sub for n in range(tok // sub)], sub)

    def held_index(r, w):
        return 3 * r + w + (1 - w) * 2 * py

    def triple(r, q, sets):
        unit(held_index(r, q // 2), sets + q % 2)

    def run(m0, m1, units, one, actions=(), more=True):
        span = m1 - m0

        @pl.loop(0, span)
        def _(j):
            exchange(m0 + j, more)
            for slot, action in actions:
                pl.when(j == slot)(action)

            @pl.loop((units * j + span - 1) // span, (units * (j + 1) + span - 1) // span)
            def _(q):
                one(q)

    run(slots, 2 * slots, 6, lambda q: triple(0, q, 0), [(4, lambda: partner_slices(0))])

    row_copy(2, cross).wait_recv()
    gate_copy(2, cross).wait_recv()
    row_copy(3, sib).start()
    gate_copy(3, sib).start()
    spread_gates(2)

    def far_rows():
        row_copy(3, sib).wait_recv()
        gate_copy(3, sib).wait_recv()
        spread_gates(3)

    run(2 * slots, 3 * slots, 12, lambda q: triple(1 - q // 6, q % 6, 2 * (q // 6)), [(2, lambda: partner_slices(1)), (4, far_rows)])
    run(3 * slots, 4 * slots - 1, 12, lambda q: triple(1 + q // 6, q % 6, 2), [(5, lambda: partner_slices(2))])
    m = 4 * slots - 1
    exchange(m)

    pl.loop(0, 2)(lambda q: unit(excl - 1, 3 - q))
    exchange(m + 1)
    partner_slices(3)

    def late(k, start, size):
        work(excl - 2, k, [start], size)

    def fold_in(n):
        at, size, slot, row, _, _ = pieces[n]
        fold_copy(n).wait_recv()

        step = min(size, h)

        @pl.loop(0, size // step)
        def _(i):
            acc[2, pl.ds(pl.multiple_of(at + i * step, step), step), :] += tmp[slot, pl.ds(pl.multiple_of(row + i * step, step), step), :]

    @pl.loop(0, 2)
    def _(n):
        late(3, n * g, g)
        part = pl.ds(pl.multiple_of(n * g, g), g)
        remote(acc.at[3, part], tmp.at[0, part], fold_ss.at[n], fold_rs.at[n], sib).start()
        late(2, n * g, g)

    late(3, *pieces[2][:2])
    fold_copy(2).start()
    fold_in(0)
    cross_copy(0).start()
    late(2, *pieces[2][:2])
    exchange(m + 2)
    fold_in(1)
    cross_copy(1).start()
    late(3, *pieces[3][:2])
    fold_copy(3).start()
    fold_in(2)
    cross_copy(2).start()
    free(freed.at[0], sib)
    late(2, *pieces[3][:2])
    fold_in(3)
    free(freed.at[1], sib)
    exchange(m + 3)

    @pl.loop(2, chunks)
    def _(c):
        late(3, c * chunk, chunk)
        late(2, c * chunk, chunk)

    for n in range(2):
        pl.semaphore_wait(freed.at[n], 1)
        fold_copy(4 + n).start()
    exchange(m + 4)
    for n in range(2):
        fold_in(4 + n)
        free(credit.at[n], cross)
    exchange(m + 5)
    for n in range(2):
        pl.semaphore_wait(credit.at[n], 1)
        cross_copy(3 + n).start()
    for n in range(len(pieces)):
        fold_copy(n).wait_send()
    free(freed.at[2], sib)

    def first_sums():
        for n in range(3):
            cross_copy(n).wait_recv()

        @pl.loop(0, 2)
        def _(i):
            part = pl.ds(pl.multiple_of(i * h, h), h)
            acc[0, part, :] += tmp[2, part, :]

        free(credit.at[2], cross)

    def last_sums():
        pl.semaphore_wait(credit.at[2], 1)
        cross_copy(5).start()

    def own(q):
        triple(2 + q // 6, q % 6, 0)

    run(m + 6, 5 * slots, 3, own)
    row_copy(3, sib).wait_send()
    hid_again = pltpu.make_async_copy(hid_ref, rows.at[3], load_sem.at[9])
    hid_again.start()
    run(5 * slots, 6 * slots, 12, lambda q: own(3 + q), [(4, first_sums), (6, last_sums)])
    run(6 * slots, 7 * slots - 1, 9, lambda q: own(15 + q), [(0, lambda: partner_slices(4)), (4, lambda: partner_slices(5))], more=False)
    last = rounds - 1
    partner_slices(last, 0, slots - 2)
    far_copy(1).start()
    exchange(count - 1, more=None, along_y=False)

    pl.loop(0, 2)(lambda q: unit(held_index(last, q), 1))
    partner_slices(last, slots - 2, slots - 1)
    far_copy(0).wait_recv()
    pl.semaphore_wait(freed.at[2], 1)

    @pl.loop(0, 2)
    def _(q):
        work(held_index(last, 2), 1, [(2 * q + n) * chunk for n in range(2)], chunk)
        last_copy(2 * q).start()
        last_copy(2 * q + 1).start()

    pl.loop(0, 3)(lambda q: unit(held_index(last, q), 0))

    @pl.loop(0, count)
    def _(m):
        up_copy(m, 1).wait_send()
        dn_copy(m, 1).wait_send()
        pl.when(m < count - 1)(lambda: y_copy(m, 2 * py).wait_send())

    far_copy(1).wait_send()

    for k, where in ((1, sib), (2, cross)):
        row_copy(k, where).wait_send()
    for k, where in ((1, sib), (2, cross), (3, sib)):
        gate_copy(k, where).wait_send()
    hid_again.wait()

    for n in range(len(pieces)):
        cross_copy(n).wait_send()
    for c in range(chunks):
        last_copy(c).wait()
        if c:
            cross_copy(c + 2).wait_recv()

        @pl.loop(0, chunk // nrm)
        def _(i):
            at = pl.ds(pl.multiple_of(c * chunk + i * nrm, nrm), nrm)
            mixed = acc[0, at, :] + acc[3, at, :]
            if c:
                mixed += tmp[(c + 2) % 3, pl.ds(pl.multiple_of(i * nrm, nrm), nrm), :]
            scale = lax.rsqrt(jnp.mean(mixed * mixed, axis=-1, keepdims=True) + EPS)
            out_ref[at, :] = (rows[3, at, :].astype(jnp.float32) + mixed * scale * post_ref[...]).astype(jnp.bfloat16)


def write_kernel(src_ref, dst_ref, sem):
    write = pltpu.make_async_copy(src_ref, dst_ref, sem)
    write.start()
    write.wait()


def solution(mesh):
    side = math.isqrt(mesh.shape['dp'])
    chips = mesh.shape['wg'] // 2

    def local_block(hidden, choice, pre_scale, w_router, w_gelu, w_linear, w_down, post_scale):
        tok, d_model = hidden.shape
        experts, _, shard = w_gelu.shape
        excl = exclusive_experts(experts)
        held = experts - excl
        count = (held // 3) * (chips - 1)
        dma = pltpu.SemaphoreType.DMA
        vmem = pl.BlockSpec(memory_space=pltpu.VMEM)
        any_space = pl.BlockSpec(memory_space=pl.ANY)
        flops = 2 * 2 * tok * experts * 3 * (chips * shard) * d_model
        out = pl.pallas_call(
            functools.partial(moe_kernel, side, chips, excl),
            out_shape=pltpu.VMEM((tok, d_model), jnp.bfloat16),
            in_specs=[any_space, vmem, vmem, vmem, any_space, any_space, any_space, any_space],
            out_specs=vmem,
            scratch_shapes=[
                pltpu.VMEM((held, chips, 3, shard, d_model), jnp.bfloat16),
                pltpu.VMEM((4, tok, d_model), jnp.bfloat16),
                pltpu.VMEM((4, tok, d_model), jnp.float32),
                pltpu.VMEM((4, experts, tok), jnp.float32),
                pltpu.VMEM((tok, 4 * experts), jnp.float32),
                pltpu.VMEM((3, tok // 4, d_model), jnp.float32),
                dma((count + 1,)), dma((count + 1,)), dma((count,)), dma((count,)), dma((count,)), dma((count,)),
                dma((11,)),
                dma((3,)), dma((3,)), dma((3,)), dma((3,)),
                dma((6,)), dma((6,)), dma((6,)), dma((6,)), dma((4,)), dma((4,)),
                pltpu.SemaphoreType.REGULAR((3,)), pltpu.SemaphoreType.REGULAR((3,)),
            ],
            compiler_params=pltpu.CompilerParams(collective_id=0, has_side_effects=True, vmem_limit_bytes=VMEM_BYTES - OUT),
            cost_estimate=pl.CostEstimate(flops=flops, bytes_accessed=8 * experts * chips * shard * d_model, transcendentals=0),
        )(hidden, choice.T, pre_scale.reshape(1, d_model), post_scale.reshape(1, d_model), w_router.T, jnp.swapaxes(w_gelu, 1, 2), jnp.swapaxes(w_linear, 1, 2), w_down)

        return pl.pallas_call(
            write_kernel,
            out_shape=jax.ShapeDtypeStruct((tok, d_model), jnp.bfloat16),
            in_specs=[vmem],
            out_specs=any_space,
            scratch_shapes=[dma(())],
        )(pltpu.with_memory_space_constraint(out, pltpu.VMEM))

    row_spec = P(('dp', 'wg'), None)
    weight_in = P(None, None, 'wg')
    return jax.shard_map(local_block, mesh=mesh, in_specs=(row_spec, row_spec, P(), P(), weight_in, weight_in, P(None, 'wg', None), P()), out_specs=row_spec, check_vma=False)
```

```python
import functools
import math

import jax
import jax.numpy as jnp
from jax import lax
from jax.experimental import pallas as pl
from jax.experimental.pallas import tpu as pltpu
from jax.sharding import PartitionSpec as P

EPS = 1e-5
MESH = pl.DeviceIdType.MESH
SUB = 256
VMEM_BYTES = 67_043_328
OUT = 2 << 20


def dot_t(lhs, rhs):
    return lax.dot_general(lhs, rhs, (((1,), (1,)), ((), ())), preferred_element_type=jnp.float32)


def exclusive_experts(experts):
    count = experts * 11 // 32
    while (experts - count) % 3:
        count -= 1
    return count


def moe_kernel(side, chips, excl, hid_ref, choice_ref, pre_ref, post_ref, router_ref, wg_ref, wl_ref, wd_ref, out_ref,
               wts, rows, acc, gate_t, gates, tmp, up_ss, up_rs, dn_ss, dn_rs, y_ss, y_rs, load_sem, row_ss, row_rs, gate_ss, gate_rs,
               fold_ss, fold_rs, cross_ss, cross_rs, part_ss, part_rs, freed, credit):
    tok, d_model = hid_ref.shape
    held, _, _, shard, _ = wts.shape
    experts = held + excl
    width = chips * shard
    slots = chips - 1
    rounds = held // 3
    count = rounds * slots
    ncol = min(256, d_model)
    chunks = 4
    chunk = tok // chunks
    sub = min(SUB, tok)

    dp, wg = lax.axis_index('dp'), lax.axis_index('wg')
    z, core = wg // 2, wg % 2
    gx, gy = dp // side, dp % side
    px, py = gx % 2, gy % 2
    up = (dp, ((z + 1) % chips) * 2 + core)
    down = (dp, ((z + chips - 1) % chips) * 2 + core)
    sib = (dp, wg + 1 - 2 * core)
    cross = (dp + side * (1 - 2 * px), wg)
    along = (dp + 1 - 2 * py, wg)

    def remote(src, dst, ss, rs, where):
        return pltpu.make_async_remote_copy(src_ref=src, dst_ref=dst, send_sem=ss, recv_sem=rs, device_id=where, device_id_type=MESH)

    def slice_copy(i, chip, ss, rs, m, where):
        ref = wts.at[i, chip]
        return remote(ref, ref, ss.at[m], rs.at[m], where)

    def up_copy(m, back):
        r, j = m // slots, m % slots
        odd, s = j % 2, j // 2 + 1
        i = 3 * r + (1 - odd) * 2 * py + odd
        return slice_copy(i, (z - s + back + chips) % chips, up_ss, up_rs, m, up)

    def dn_copy(m, back):
        r, j = m // slots, m % slots
        odd, s = j % 2, j // 2 + 1
        i = 3 * r + odd * 2 * py + (1 - odd)
        return slice_copy(i, (z + s - back) % chips, dn_ss, dn_rs, m, down)

    def y_copy(m, i):
        r, j = m // slots, m % slots
        odd, s = j % 2, j // 2 + 1
        return slice_copy(3 * r + i, (z + (2 * odd - 1) * s + chips) % chips, y_ss, y_rs, m, along)

    def exchange(m, more=True, along_y=True):
        up_copy(m, 0).wait_recv()
        if more is True:
            up_copy(m + 2, 1).start()
        else:
            pl.when(m + 2 < count)(lambda: up_copy(m + 2, 1).start())
        dn_copy(m, 0).wait_recv()
        if more is True:
            dn_copy(m + 2, 1).start()
        else:
            pl.when(m + 2 < count)(lambda: dn_copy(m + 2, 1).start())
        if along_y:
            y_copy(m, 2 * py).start()

    def partner_slices(r, first=0, end=slots):
        @pl.loop(first, end)
        def _(k):
            y_copy(r * slots + k, 2 - 2 * py).wait_recv()

    def far_copy(back):
        return slice_copy(3 * (rounds - 1) + 2 - 2 * py, (z - chips // 2 + back + chips) % chips, up_ss, up_rs, count, up)

    def row_copy(k, where):
        return remote(rows.at[0] if k < 3 else rows.at[2], rows.at[k], row_ss.at[k - 1], row_rs.at[k - 1], where)

    def gate_copy(k, where):
        return remote(gate_t.at[0] if k < 3 else gate_t.at[2], gate_t.at[k], gate_ss.at[k - 1], gate_rs.at[k - 1], where)

    def part_of(c):
        return pl.ds(pl.multiple_of(c * chunk, chunk), chunk)

    h = chunk // 2
    pieces = ((0, h, 0, 0, 2, 0), (h, h, 0, h, 2, h), (chunk, chunk, 1, 0, 0, 0), (2 * chunk, chunk, 0, 0, 1, 0), (3 * chunk, chunk, 1, 0, 2, 0))

    def fold_copy(n):
        at, size, slot, row, _, _ = pieces[n]
        return remote(acc.at[3, pl.ds(at, size)], tmp.at[slot, pl.ds(row, size)], fold_ss.at[n], fold_rs.at[n], sib)

    def cross_copy(n):
        at, size, _, _, slot, row = pieces[n]
        return remote(acc.at[2, pl.ds(at, size)], tmp.at[slot, pl.ds(row, size)], cross_ss.at[n], cross_rs.at[n], cross)

    def free(sem, where):
        pl.semaphore_signal(sem, inc=1, device_id=where, device_id_type=MESH)

    def last_copy(c):
        at = part_of(c)
        return remote(acc.at[1, at], acc.at[3, at], part_ss.at[c], part_rs.at[c], sib)

    loads = []
    for n, (src0, dst0, size) in enumerate(((px * excl, 0, 3), (px * excl + 3, 3, excl - 3), (2 * excl, excl, held - excl))):
        for k, src in enumerate((wg_ref, wl_ref, wd_ref)):
            loads.append(pltpu.make_async_copy(src.at[pl.ds(src0, size)], wts.at[pl.ds(dst0, size), z, k], load_sem.at[3 * n + k]))
    hid_load = pltpu.make_async_copy(hid_ref, rows.at[0], load_sem.at[9])
    router_load = pltpu.make_async_copy(router_ref, out_ref.at[pl.ds(0, experts)], load_sem.at[10])
    for load in loads[:3] + [hid_load, router_load] + loads[3:]:
        load.start()

    barrier = pltpu.get_barrier_semaphore()
    for peer in (up, down, sib, cross, along):
        pl.semaphore_signal(barrier, inc=1, device_id=peer, device_id_type=MESH)
    pl.semaphore_wait(barrier, 5)

    for load in loads[:3]:
        load.wait()
    for m in range(2):
        up_copy(m, 1).start()
        dn_copy(m, 1).start()

    nrm = min(128, chunk)

    @pl.loop(0, 4 * tok // nrm)
    def _(i):
        at = pl.ds(pl.multiple_of((i // 4) * nrm, nrm), nrm)
        acc[i % 4, at, :] = jnp.zeros((nrm, d_model), jnp.float32)

    hid_load.wait()

    @pl.loop(0, tok // nrm)
    def _(i):
        at = pl.ds(pl.multiple_of(i * nrm, nrm), nrm)
        values = rows[0, at, :].astype(jnp.float32)
        scale = lax.rsqrt(jnp.mean(values * values, axis=-1, keepdims=True) + EPS)
        rows[0, at, :] = (values * scale * pre_ref[...]).astype(jnp.bfloat16)

    for load in loads[3:]:
        load.wait()

    router_load.wait()
    rtr = min(256, tok)

    @pl.loop(0, tok // rtr)
    def _(i):
        at = pl.ds(pl.multiple_of(i * rtr, rtr), rtr)
        logits = dot_t(out_ref[pl.ds(0, experts), :], rows[0, at, :])
        shifted = jnp.exp(logits - jnp.max(logits, axis=0, keepdims=True))
        probs = shifted / jnp.sum(shifted, axis=0, keepdims=True)
        expert_ids = lax.broadcasted_iota(jnp.int32, (experts, rtr), 0)
        picks = choice_ref[:, at]
        chosen = expert_ids == picks[0:1, :]
        for j in range(1, picks.shape[0]):
            chosen = chosen | (expert_ids == picks[j:j + 1, :])
        gate_t[0, :, at] = jnp.where(chosen, probs, -1.0)

    for k, where in ((2, cross), (1, sib)):
        gate_copy(k, where).start()
        row_copy(k, where).start()

    def spread_gates(k):
        gates[:, k * experts:(k + 1) * experts] = gate_t[k].T

    spread_gates(0)

    @pl.loop(0, slots)
    def _(j):
        exchange(j)

    row_copy(1, sib).wait_recv()
    gate_copy(1, sib).wait_recv()
    spread_gates(1)

    def work(i, k, starts, size):
        e = i + excl * (px + (1 - px) * jnp.minimum(i // excl, 1)) + k * experts
        lane = lax.broadcasted_iota(jnp.int32, (size, 4 * experts), 1)
        c = math.sqrt(2.0 / math.pi)
        acts = []
        for start in starts:
            at = pl.ds(pl.multiple_of(start, size), size)
            x = rows[k, at, :]
            u = dot_t(x, wts[i, :, 0].reshape(width, d_model))
            v = dot_t(x, wts[i, :, 1].reshape(width, d_model))
            gate = jnp.sum(jnp.where(lane == e, gates[at, :], 0.0), axis=1, keepdims=True)
            cdf = 0.5 * (1.0 + jnp.tanh(c * (u + 0.044715 * (u * u * u))))
            acts.append((at, gate, jnp.where(gate >= 0.0, u * cdf * v, 0.0).astype(jnp.bfloat16)))
        for at, gate, a in acts:
            for n in range(d_model // ncol):
                cols = pl.ds(n * ncol, ncol)
                o = jnp.dot(a, wts[i, :, 2, :, cols].reshape(width, ncol), preferred_element_type=jnp.float32)
                acc[k, at, cols] += gate * o

    def unit(i, k):
        work(i, k, [n * sub for n in range(tok // sub)], sub)

    def held_index(r, w):
        return 3 * r + w + (1 - w) * 2 * py

    def triple(r, q, sets):
        unit(held_index(r, q // 2), sets + q % 2)

    def run(m0, m1, units, one, actions=(), more=True):
        span = m1 - m0

        @pl.loop(0, span)
        def _(j):
            exchange(m0 + j, more)
            for slot, action in actions:
                pl.when(j == slot)(action)

            @pl.loop((units * j + span - 1) // span, (units * (j + 1) + span - 1) // span)
            def _(q):
                one(q)

    run(slots, 2 * slots, 6, lambda q: triple(0, q, 0), [(4, lambda: partner_slices(0))])

    row_copy(2, cross).wait_recv()
    gate_copy(2, cross).wait_recv()
    row_copy(3, sib).start()
    gate_copy(3, sib).start()
    spread_gates(2)

    def far_rows():
        row_copy(3, sib).wait_recv()
        gate_copy(3, sib).wait_recv()
        spread_gates(3)

    run(2 * slots, 3 * slots, 12, lambda q: triple(1 - q // 6, q % 6, 2 * (q // 6)), [(2, lambda: partner_slices(1)), (4, far_rows)])
    run(3 * slots, 4 * slots - 1, 12, lambda q: triple(1 + q // 6, q % 6, 2), [(5, lambda: partner_slices(2))])
    m = 4 * slots - 1
    exchange(m)

    pl.loop(0, 2)(lambda q: unit(excl - 1, 3 - q))
    exchange(m + 1)
    pl.when(py == 1)(lambda: partner_slices(3))

    def late(k, start, size):
        work(excl - 2, k, [start], size)

    def fold_in(n):
        at, size, slot, row, _, _ = pieces[n]
        fold_copy(n).wait_recv()

        @pl.loop(0, size // h)
        def _(i):
            acc[2, pl.ds(pl.multiple_of(at + i * h, h), h), :] += tmp[slot, pl.ds(pl.multiple_of(row + i * h, h), h), :]

    @pl.loop(0, 2)
    def _(n):
        late(3, n * h, h)
        part = pl.ds(pl.multiple_of(n * h, h), h)
        remote(acc.at[3, part], tmp.at[0, part], fold_ss.at[n], fold_rs.at[n], sib).start()
        late(2, n * h, h)

    late(3, *pieces[2][:2])
    fold_copy(2).start()
    fold_in(0)
    cross_copy(0).start()
    exchange(m + 2)
    late(2, *pieces[2][:2])
    fold_in(1)
    cross_copy(1).start()
    free(freed.at[0], sib)
    fold_in(2)
    free(freed.at[1], sib)

    exchange(m + 3)

    @pl.loop(2, chunks)
    def _(c):
        late(3, c * chunk, chunk)
        late(2, c * chunk, chunk)

    for n in range(2):
        pl.semaphore_wait(freed.at[n], 1)
        fold_copy(3 + n).start()
    exchange(m + 4)
    for n in range(2):
        fold_in(3 + n)
        free(credit.at[n], cross)
    exchange(m + 5)
    for n in range(2):
        pl.semaphore_wait(credit.at[n], 1)
        cross_copy(2 + n).start()
    for n in range(len(pieces)):
        fold_copy(n).wait_send()
    free(freed.at[2], sib)

    def first_sums():
        for n in range(2):
            cross_copy(n).wait_recv()

        @pl.loop(0, 2)
        def _(i):
            part = pl.ds(pl.multiple_of(i * h, h), h)
            acc[0, part, :] += tmp[2, part, :]

        free(credit.at[2], cross)

    def last_sums():
        pl.semaphore_wait(credit.at[2], 1)
        cross_copy(4).start()

    def own(q):
        triple(2 + q // 6, q % 6, 0)

    run(m + 6, 5 * slots, 3, own)
    row_copy(3, sib).wait_send()
    hid_again = pltpu.make_async_copy(hid_ref, rows.at[3], load_sem.at[9])
    hid_again.start()
    run(5 * slots, 6 * slots, 12, lambda q: own(3 + q), [(0, lambda: pl.when(py == 0)(lambda: partner_slices(3))), (4, first_sums), (6, last_sums)])
    run(6 * slots, 7 * slots - 1, 9, lambda q: own(15 + q), [(0, lambda: partner_slices(4)), (4, lambda: partner_slices(5))], more=False)
    last = rounds - 1
    partner_slices(last, 0, slots - 2)
    far_copy(1).start()
    exchange(count - 1, more=None, along_y=False)

    pl.loop(0, 2)(lambda q: unit(held_index(last, q), 1))
    partner_slices(last, slots - 2, slots - 1)
    far_copy(0).wait_recv()
    pl.semaphore_wait(freed.at[2], 1)

    @pl.loop(0, 2)
    def _(q):
        work(held_index(last, 2), 1, [(2 * q + n) * chunk for n in range(2)], chunk)
        last_copy(2 * q).start()
        last_copy(2 * q + 1).start()

    pl.loop(0, 3)(lambda q: unit(held_index(last, q), 0))

    @pl.loop(0, count)
    def _(m):
        up_copy(m, 1).wait_send()
        dn_copy(m, 1).wait_send()
        pl.when(m < count - 1)(lambda: y_copy(m, 2 * py).wait_send())

    far_copy(1).wait_send()

    for k, where in ((1, sib), (2, cross)):
        row_copy(k, where).wait_send()
    for k, where in ((1, sib), (2, cross), (3, sib)):
        gate_copy(k, where).wait_send()
    hid_again.wait()

    for n in range(len(pieces)):
        cross_copy(n).wait_send()
    for c in range(chunks):
        last_copy(c).wait()
        if c:
            cross_copy(c + 1).wait_recv()

        @pl.loop(0, chunk // nrm)
        def _(i):
            at = pl.ds(pl.multiple_of(c * chunk + i * nrm, nrm), nrm)
            mixed = acc[0, at, :] + acc[3, at, :]
            if c:
                mixed += tmp[(c + 2) % 3, pl.ds(pl.multiple_of(i * nrm, nrm), nrm), :]
            scale = lax.rsqrt(jnp.mean(mixed * mixed, axis=-1, keepdims=True) + EPS)
            out_ref[at, :] = (rows[3, at, :].astype(jnp.float32) + mixed * scale * post_ref[...]).astype(jnp.bfloat16)


def write_kernel(src_ref, dst_ref, sem):
    write = pltpu.make_async_copy(src_ref, dst_ref, sem)
    write.start()
    write.wait()


def solution(mesh):
    side = math.isqrt(mesh.shape['dp'])
    chips = mesh.shape['wg'] // 2

    def local_block(hidden, choice, pre_scale, w_router, w_gelu, w_linear, w_down, post_scale):
        tok, d_model = hidden.shape
        experts, _, shard = w_gelu.shape
        excl = exclusive_experts(experts)
        held = experts - excl
        count = (held // 3) * (chips - 1)
        dma = pltpu.SemaphoreType.DMA
        vmem = pl.BlockSpec(memory_space=pltpu.VMEM)
        any_space = pl.BlockSpec(memory_space=pl.ANY)
        flops = 2 * 2 * tok * experts * 3 * (chips * shard) * d_model
        out = pl.pallas_call(
            functools.partial(moe_kernel, side, chips, excl),
            out_shape=pltpu.VMEM((tok, d_model), jnp.bfloat16),
            in_specs=[any_space, vmem, vmem, vmem, any_space, any_space, any_space, any_space],
            out_specs=vmem,
            scratch_shapes=[
                pltpu.VMEM((held, chips, 3, shard, d_model), jnp.bfloat16),
                pltpu.VMEM((4, tok, d_model), jnp.bfloat16),
                pltpu.VMEM((4, tok, d_model), jnp.float32),
                pltpu.VMEM((4, experts, tok), jnp.float32),
                pltpu.VMEM((tok, 4 * experts), jnp.float32),
                pltpu.VMEM((3, tok // 4, d_model), jnp.float32),
                dma((count + 1,)), dma((count + 1,)), dma((count,)), dma((count,)), dma((count,)), dma((count,)),
                dma((11,)),
                dma((3,)), dma((3,)), dma((3,)), dma((3,)),
                dma((5,)), dma((5,)), dma((5,)), dma((5,)), dma((4,)), dma((4,)),
                pltpu.SemaphoreType.REGULAR((3,)), pltpu.SemaphoreType.REGULAR((3,)),
            ],
            compiler_params=pltpu.CompilerParams(collective_id=0, has_side_effects=True, vmem_limit_bytes=VMEM_BYTES - OUT),
            cost_estimate=pl.CostEstimate(flops=flops, bytes_accessed=8 * experts * chips * shard * d_model, transcendentals=0),
        )(hidden, choice.T, pre_scale.reshape(1, d_model), post_scale.reshape(1, d_model), w_router.T, jnp.swapaxes(w_gelu, 1, 2), jnp.swapaxes(w_linear, 1, 2), w_down)

        return pl.pallas_call(
            write_kernel,
            out_shape=jax.ShapeDtypeStruct((tok, d_model), jnp.bfloat16),
            in_specs=[vmem],
            out_specs=any_space,
            scratch_shapes=[dma(())],
        )(pltpu.with_memory_space_constraint(out, pltpu.VMEM))

    row_spec = P(('dp', 'wg'), None)
    weight_in = P(None, None, 'wg')
    return jax.shard_map(local_block, mesh=mesh, in_specs=(row_spec, row_spec, P(), P(), weight_in, weight_in, P(None, 'wg', None), P()), out_specs=row_spec, check_vma=False)
```

```python
import functools
import math

import jax
import jax.numpy as jnp
from jax import lax
from jax.experimental import pallas as pl
from jax.experimental.pallas import tpu as pltpu
from jax.sharding import PartitionSpec as P

EPS = 1e-5
MESH = pl.DeviceIdType.MESH
SUB = 256
VMEM_BYTES = 67_043_328
OUT = 2 << 20


def dot_t(lhs, rhs):
    return lax.dot_general(lhs, rhs, (((1,), (1,)), ((), ())), preferred_element_type=jnp.float32)


def exclusive_experts(experts):
    count = experts * 11 // 32
    while (experts - count) % 3:
        count -= 1
    return count


def moe_kernel(side, chips, excl, hid_ref, choice_ref, pre_ref, post_ref, router_ref, wg_ref, wl_ref, wd_ref, out_ref,
               wts, rows, acc, gate_t, gates, tmp, up_ss, up_rs, dn_ss, dn_rs, y_ss, y_rs, load_sem, row_ss, row_rs, gate_ss, gate_rs,
               fold_ss, fold_rs, cross_ss, cross_rs, part_ss, part_rs, freed, credit):
    tok, d_model = hid_ref.shape
    held, _, _, shard, _ = wts.shape
    experts = held + excl
    width = chips * shard
    slots = chips - 1
    rounds = held // 3
    count = rounds * slots
    ncol = min(256, d_model)
    chunks = 4
    chunk = tok // chunks
    sub = min(SUB, tok)

    dp, wg = lax.axis_index('dp'), lax.axis_index('wg')
    z, core = wg // 2, wg % 2
    gx, gy = dp // side, dp % side
    px, py = gx % 2, gy % 2
    up = (dp, ((z + 1) % chips) * 2 + core)
    down = (dp, ((z + chips - 1) % chips) * 2 + core)
    sib = (dp, wg + 1 - 2 * core)
    cross = (dp + side * (1 - 2 * px), wg)
    along = (dp + 1 - 2 * py, wg)

    def remote(src, dst, ss, rs, where):
        return pltpu.make_async_remote_copy(src_ref=src, dst_ref=dst, send_sem=ss, recv_sem=rs, device_id=where, device_id_type=MESH)

    def slice_copy(i, chip, ss, rs, m, where):
        ref = wts.at[i, chip]
        return remote(ref, ref, ss.at[m], rs.at[m], where)

    def up_copy(m, back):
        r, j = m // slots, m % slots
        odd, s = j % 2, j // 2 + 1
        i = 3 * r + (1 - odd) * 2 * py + odd
        return slice_copy(i, (z - s + back + chips) % chips, up_ss, up_rs, m, up)

    def dn_copy(m, back):
        r, j = m // slots, m % slots
        odd, s = j % 2, j // 2 + 1
        i = 3 * r + odd * 2 * py + (1 - odd)
        return slice_copy(i, (z + s - back) % chips, dn_ss, dn_rs, m, down)

    def y_copy(m, i):
        r, j = m // slots, m % slots
        odd, s = j % 2, j // 2 + 1
        return slice_copy(3 * r + i, (z + (2 * odd - 1) * s + chips) % chips, y_ss, y_rs, m, along)

    def exchange(m, more=True, along_y=True):
        up_copy(m, 0).wait_recv()
        if more is True:
            up_copy(m + 2, 1).start()
        else:
            pl.when(m + 2 < count)(lambda: up_copy(m + 2, 1).start())
        odd = (m % slots) % 2
        if along_y:
            pl.when(odd == 0)(lambda: y_copy(m, 2 * py).start())
        dn_copy(m, 0).wait_recv()
        if more is True:
            dn_copy(m + 2, 1).start()
        else:
            pl.when(m + 2 < count)(lambda: dn_copy(m + 2, 1).start())
        if along_y:
            pl.when(odd == 1)(lambda: y_copy(m, 2 * py).start())

    def partner_slices(r, first=0, end=slots):
        @pl.loop(first, end)
        def _(k):
            y_copy(r * slots + k, 2 - 2 * py).wait_recv()

    def far_copy(back):
        return slice_copy(3 * (rounds - 1) + 2 - 2 * py, (z - chips // 2 + back + chips) % chips, up_ss, up_rs, count, up)

    def row_copy(k, where):
        return remote(rows.at[0] if k < 3 else rows.at[2], rows.at[k], row_ss.at[k - 1], row_rs.at[k - 1], where)

    def gate_copy(k, where):
        return remote(gate_t.at[0] if k < 3 else gate_t.at[2], gate_t.at[k], gate_ss.at[k - 1], gate_rs.at[k - 1], where)

    def part_of(c):
        return pl.ds(pl.multiple_of(c * chunk, chunk), chunk)

    h = chunk // 2
    pieces = ((0, h, 0, 0, 2, 0), (h, h, 0, h, 2, h), (chunk, chunk, 1, 0, 0, 0), (2 * chunk, chunk, 0, 0, 1, 0), (3 * chunk, chunk, 1, 0, 2, 0))

    def fold_copy(n):
        at, size, slot, row, _, _ = pieces[n]
        return remote(acc.at[3, pl.ds(at, size)], tmp.at[slot, pl.ds(row, size)], fold_ss.at[n], fold_rs.at[n], sib)

    def cross_copy(n):
        at, size, _, _, slot, row = pieces[n]
        return remote(acc.at[2, pl.ds(at, size)], tmp.at[slot, pl.ds(row, size)], cross_ss.at[n], cross_rs.at[n], cross)

    def free(sem, where):
        pl.semaphore_signal(sem, inc=1, device_id=where, device_id_type=MESH)

    def last_copy(c):
        at = part_of(c)
        return remote(acc.at[1, at], acc.at[3, at], part_ss.at[c], part_rs.at[c], sib)

    loads = []
    for n, (src0, dst0, size) in enumerate(((px * excl, 0, 3), (px * excl + 3, 3, excl - 3), (2 * excl, excl, held - excl))):
        for k, src in enumerate((wg_ref, wl_ref, wd_ref)):
            loads.append(pltpu.make_async_copy(src.at[pl.ds(src0, size)], wts.at[pl.ds(dst0, size), z, k], load_sem.at[3 * n + k]))
    hid_load = pltpu.make_async_copy(hid_ref, rows.at[0], load_sem.at[9])
    router_load = pltpu.make_async_copy(router_ref, out_ref.at[pl.ds(0, experts)], load_sem.at[10])
    for load in loads[:3] + [hid_load, router_load] + loads[3:]:
        load.start()

    barrier = pltpu.get_barrier_semaphore()
    for peer in (up, down, sib, cross, along):
        pl.semaphore_signal(barrier, inc=1, device_id=peer, device_id_type=MESH)
    pl.semaphore_wait(barrier, 5)

    for load in loads[:3]:
        load.wait()
    for m in range(2):
        up_copy(m, 1).start()
        dn_copy(m, 1).start()

    nrm = min(128, chunk)

    @pl.loop(0, 4 * tok // nrm)
    def _(i):
        at = pl.ds(pl.multiple_of((i // 4) * nrm, nrm), nrm)
        acc[i % 4, at, :] = jnp.zeros((nrm, d_model), jnp.float32)

    hid_load.wait()

    @pl.loop(0, tok // nrm)
    def _(i):
        at = pl.ds(pl.multiple_of(i * nrm, nrm), nrm)
        values = rows[0, at, :].astype(jnp.float32)
        scale = lax.rsqrt(jnp.mean(values * values, axis=-1, keepdims=True) + EPS)
        rows[0, at, :] = (values * scale * pre_ref[...]).astype(jnp.bfloat16)

    for load in loads[3:]:
        load.wait()

    router_load.wait()
    rtr = min(256, tok)

    @pl.loop(0, tok // rtr)
    def _(i):
        at = pl.ds(pl.multiple_of(i * rtr, rtr), rtr)
        logits = dot_t(out_ref[pl.ds(0, experts), :], rows[0, at, :])
        shifted = jnp.exp(logits - jnp.max(logits, axis=0, keepdims=True))
        probs = shifted / jnp.sum(shifted, axis=0, keepdims=True)
        expert_ids = lax.broadcasted_iota(jnp.int32, (experts, rtr), 0)
        picks = choice_ref[:, at]
        chosen = expert_ids == picks[0:1, :]
        for j in range(1, picks.shape[0]):
            chosen = chosen | (expert_ids == picks[j:j + 1, :])
        gate_t[0, :, at] = jnp.where(chosen, probs, -1.0)

    for k, where in ((2, cross), (1, sib)):
        gate_copy(k, where).start()
        row_copy(k, where).start()

    def spread_gates(k):
        gates[:, k * experts:(k + 1) * experts] = gate_t[k].T

    spread_gates(0)

    @pl.loop(0, slots)
    def _(j):
        exchange(j)

    row_copy(1, sib).wait_recv()
    gate_copy(1, sib).wait_recv()
    spread_gates(1)

    def work(i, k, starts, size):
        e = i + excl * (px + (1 - px) * jnp.minimum(i // excl, 1)) + k * experts
        lane = lax.broadcasted_iota(jnp.int32, (size, 4 * experts), 1)
        c = math.sqrt(2.0 / math.pi)
        acts = []
        for start in starts:
            at = pl.ds(pl.multiple_of(start, size), size)
            x = rows[k, at, :]
            u = dot_t(x, wts[i, :, 0].reshape(width, d_model))
            v = dot_t(x, wts[i, :, 1].reshape(width, d_model))
            gate = jnp.sum(jnp.where(lane == e, gates[at, :], 0.0), axis=1, keepdims=True)
            cdf = 0.5 * (1.0 + jnp.tanh(c * (u + 0.044715 * (u * u * u))))
            acts.append((at, gate, jnp.where(gate >= 0.0, u * cdf * v, 0.0).astype(jnp.bfloat16)))
        for at, gate, a in acts:
            for n in range(d_model // ncol):
                cols = pl.ds(n * ncol, ncol)
                o = jnp.dot(a, wts[i, :, 2, :, cols].reshape(width, ncol), preferred_element_type=jnp.float32)
                acc[k, at, cols] += gate * o

    def unit(i, k):
        work(i, k, [n * sub for n in range(tok // sub)], sub)

    def held_index(r, w):
        return 3 * r + w + (1 - w) * 2 * py

    def triple(r, q, sets):
        unit(held_index(r, q // 2), sets + q % 2)

    def run(m0, m1, units, one, actions=(), more=True):
        span = m1 - m0

        @pl.loop(0, span)
        def _(j):
            exchange(m0 + j, more)
            for slot, action in actions:
                pl.when(j == slot)(action)

            @pl.loop((units * j + span - 1) // span, (units * (j + 1) + span - 1) // span)
            def _(q):
                one(q)

    run(slots, 2 * slots, 6, lambda q: triple(0, q, 0), [(4, lambda: partner_slices(0))])

    row_copy(2, cross).wait_recv()
    gate_copy(2, cross).wait_recv()
    row_copy(3, sib).start()
    gate_copy(3, sib).start()
    spread_gates(2)

    def far_rows():
        row_copy(3, sib).wait_recv()
        gate_copy(3, sib).wait_recv()
        spread_gates(3)

    run(2 * slots, 3 * slots, 12, lambda q: triple(1 - q // 6, q % 6, 2 * (q // 6)), [(2, lambda: partner_slices(1)), (4, far_rows)])
    run(3 * slots, 4 * slots - 1, 12, lambda q: triple(1 + q // 6, q % 6, 2), [(5, lambda: partner_slices(2))])
    m = 4 * slots - 1
    exchange(m)

    pl.loop(0, 2)(lambda q: unit(excl - 1, 3 - q))
    exchange(m + 1)
    partner_slices(3)

    def late(k, start, size):
        work(excl - 2, k, [start], size)

    def fold_in(n):
        at, size, slot, row, _, _ = pieces[n]
        fold_copy(n).wait_recv()

        @pl.loop(0, size // h)
        def _(i):
            acc[2, pl.ds(pl.multiple_of(at + i * h, h), h), :] += tmp[slot, pl.ds(pl.multiple_of(row + i * h, h), h), :]

    @pl.loop(0, 2)
    def _(n):
        late(3, n * h, h)
        part = pl.ds(pl.multiple_of(n * h, h), h)
        remote(acc.at[3, part], tmp.at[0, part], fold_ss.at[n], fold_rs.at[n], sib).start()
        late(2, n * h, h)

    late(3, *pieces[2][:2])
    fold_copy(2).start()
    fold_in(0)
    cross_copy(0).start()
    exchange(m + 2)
    late(2, *pieces[2][:2])
    fold_in(1)
    cross_copy(1).start()
    free(freed.at[0], sib)
    fold_in(2)
    free(freed.at[1], sib)

    exchange(m + 3)

    @pl.loop(2, chunks)
    def _(c):
        late(3, c * chunk, chunk)
        late(2, c * chunk, chunk)

    for n in range(2):
        pl.semaphore_wait(freed.at[n], 1)
        fold_copy(3 + n).start()
    exchange(m + 4)
    for n in range(2):
        fold_in(3 + n)
        free(credit.at[n], cross)
    exchange(m + 5)
    for n in range(2):
        pl.semaphore_wait(credit.at[n], 1)
        cross_copy(2 + n).start()
    for n in range(len(pieces)):
        fold_copy(n).wait_send()
    free(freed.at[2], sib)

    def first_sums():
        for n in range(2):
            cross_copy(n).wait_recv()

        @pl.loop(0, 2)
        def _(i):
            part = pl.ds(pl.multiple_of(i * h, h), h)
            acc[0, part, :] += tmp[2, part, :]

        free(credit.at[2], cross)

    def last_sums():
        pl.semaphore_wait(credit.at[2], 1)
        cross_copy(4).start()

    def own(q):
        triple(2 + q // 6, q % 6, 0)

    run(m + 6, 5 * slots, 3, own)
    row_copy(3, sib).wait_send()
    hid_again = pltpu.make_async_copy(hid_ref, rows.at[3], load_sem.at[9])
    hid_again.start()
    run(5 * slots, 6 * slots, 12, lambda q: own(3 + q), [(4, first_sums), (6, last_sums)])
    run(6 * slots, 7 * slots - 1, 9, lambda q: own(15 + q), [(0, lambda: partner_slices(4)), (4, lambda: partner_slices(5))], more=False)
    last = rounds - 1
    partner_slices(last, 0, slots - 2)
    far_copy(1).start()
    exchange(count - 1, more=None, along_y=False)

    pl.loop(0, 2)(lambda q: unit(held_index(last, q), 1))
    partner_slices(last, slots - 2, slots - 1)
    far_copy(0).wait_recv()
    pl.semaphore_wait(freed.at[2], 1)

    @pl.loop(0, 2)
    def _(q):
        work(held_index(last, 2), 1, [(2 * q + n) * chunk for n in range(2)], chunk)
        last_copy(2 * q).start()
        last_copy(2 * q + 1).start()

    pl.loop(0, 3)(lambda q: unit(held_index(last, q), 0))

    @pl.loop(0, count)
    def _(m):
        up_copy(m, 1).wait_send()
        dn_copy(m, 1).wait_send()
        pl.when(m < count - 1)(lambda: y_copy(m, 2 * py).wait_send())

    far_copy(1).wait_send()

    for k, where in ((1, sib), (2, cross)):
        row_copy(k, where).wait_send()
    for k, where in ((1, sib), (2, cross), (3, sib)):
        gate_copy(k, where).wait_send()
    hid_again.wait()

    for n in range(len(pieces)):
        cross_copy(n).wait_send()
    for c in range(chunks):
        last_copy(c).wait()
        if c:
            cross_copy(c + 1).wait_recv()

        @pl.loop(0, chunk // nrm)
        def _(i):
            at = pl.ds(pl.multiple_of(c * chunk + i * nrm, nrm), nrm)
            mixed = acc[0, at, :] + acc[3, at, :]
            if c:
                mixed += tmp[(c + 2) % 3, pl.ds(pl.multiple_of(i * nrm, nrm), nrm), :]
            scale = lax.rsqrt(jnp.mean(mixed * mixed, axis=-1, keepdims=True) + EPS)
            out_ref[at, :] = (rows[3, at, :].astype(jnp.float32) + mixed * scale * post_ref[...]).astype(jnp.bfloat16)


def write_kernel(src_ref, dst_ref, sem):
    write = pltpu.make_async_copy(src_ref, dst_ref, sem)
    write.start()
    write.wait()


def solution(mesh):
    side = math.isqrt(mesh.shape['dp'])
    chips = mesh.shape['wg'] // 2

    def local_block(hidden, choice, pre_scale, w_router, w_gelu, w_linear, w_down, post_scale):
        tok, d_model = hidden.shape
        experts, _, shard = w_gelu.shape
        excl = exclusive_experts(experts)
        held = experts - excl
        count = (held // 3) * (chips - 1)
        dma = pltpu.SemaphoreType.DMA
        vmem = pl.BlockSpec(memory_space=pltpu.VMEM)
        any_space = pl.BlockSpec(memory_space=pl.ANY)
        flops = 2 * 2 * tok * experts * 3 * (chips * shard) * d_model
        out = pl.pallas_call(
            functools.partial(moe_kernel, side, chips, excl),
            out_shape=pltpu.VMEM((tok, d_model), jnp.bfloat16),
            in_specs=[any_space, vmem, vmem, vmem, any_space, any_space, any_space, any_space],
            out_specs=vmem,
            scratch_shapes=[
                pltpu.VMEM((held, chips, 3, shard, d_model), jnp.bfloat16),
                pltpu.VMEM((4, tok, d_model), jnp.bfloat16),
                pltpu.VMEM((4, tok, d_model), jnp.float32),
                pltpu.VMEM((4, experts, tok), jnp.float32),
                pltpu.VMEM((tok, 4 * experts), jnp.float32),
                pltpu.VMEM((3, tok // 4, d_model), jnp.float32),
                dma((count + 1,)), dma((count + 1,)), dma((count,)), dma((count,)), dma((count,)), dma((count,)),
                dma((11,)),
                dma((3,)), dma((3,)), dma((3,)), dma((3,)),
                dma((5,)), dma((5,)), dma((5,)), dma((5,)), dma((4,)), dma((4,)),
                pltpu.SemaphoreType.REGULAR((3,)), pltpu.SemaphoreType.REGULAR((3,)),
            ],
            compiler_params=pltpu.CompilerParams(collective_id=0, has_side_effects=True, vmem_limit_bytes=VMEM_BYTES - OUT),
            cost_estimate=pl.CostEstimate(flops=flops, bytes_accessed=8 * experts * chips * shard * d_model, transcendentals=0),
        )(hidden, choice.T, pre_scale.reshape(1, d_model), post_scale.reshape(1, d_model), w_router.T, jnp.swapaxes(w_gelu, 1, 2), jnp.swapaxes(w_linear, 1, 2), w_down)

        return pl.pallas_call(
            write_kernel,
            out_shape=jax.ShapeDtypeStruct((tok, d_model), jnp.bfloat16),
            in_specs=[vmem],
            out_specs=any_space,
            scratch_shapes=[dma(())],
        )(pltpu.with_memory_space_constraint(out, pltpu.VMEM))

    row_spec = P(('dp', 'wg'), None)
    weight_in = P(None, None, 'wg')
    return jax.shard_map(local_block, mesh=mesh, in_specs=(row_spec, row_spec, P(), P(), weight_in, weight_in, P(None, 'wg', None), P()), out_specs=row_spec, check_vma=False)
```
